512 devices in a mesh: parts: 2 (over y), section: 4 (over x), tile: 64 (over z, core).
Axes of the slice: x: 4, y: 2, z: 32, core: 2. Of those that a mesh axis runs over, the one named last changes fastest.
The devices are a block of a 4x8x32 slice.
Arguments:
- frames: bfloat16 [8, 64, 16, 16, 128], P('parts', 'tile'), parts along dimension 0, may hold values from -8 to 8
- cache: bfloat16 [4, 4, 64, 16, 16, 128], P('section', 'parts', 'tile'), parts along dimension 1, may hold values from -4 to 4
- conv_weight: bfloat16 [4, 3, 3, 3, 128, 128], P('section'), may hold values from -0.109375 to 0.109375
- conv_bias: float32 [4, 128], P('section'), may hold values from -2 to 2
- norm_gain: float32 [4, 128], P('section'), may hold values from 0.1 to 1.9
- norm_bias: float32 [4, 128], P('section'), may hold values from -2 to 2
Outputs:
- section_outputs: bfloat16 [4, 8, 64, 16, 16, 128], P('section', 'parts', 'tile'), parts along dimension 1
The draws below stay inside these ranges and needn't reach their ends.
There are 2 independent parts, one for each index of `parts`. The reference program is written for one: setup_inputs(seed, part) draws one part's arguments, and reference() takes and returns one part's arrays. A program takes and returns all parts, laid end to end along the dimension named above; an argument that names none is the same for every part. Nothing has to cross between parts.
All inputs are finite; a program needn't handle non-finite values.
Results may differ from the reference program's by a relative error of at most 0.0056.
Values may be sent and summed in bfloat16 or wider, within the bound.
No kernel may reach another device: no remote copies, remote signals or barrier semaphores. Data moves between devices by JAX's collectives and lax.ppermute only.
A program may use at most 64 MiB of HBM per device.

```python
import jax
import jax.numpy as jnp
from jax import lax

C = 128
GROUPS = 32
F = 4
TH = 16
TW = 16
CTX = 2
GX = 8
GY = 8
N_SECTION = 4
N_TILE = 64


def draw_frames(key, part):
    first, second, third = jax.random.split(jax.random.fold_in(key, 11), 3)
    shape = (F, N_TILE, TH, TW, C)
    position = jnp.arange(N_TILE, dtype=jnp.float32) / max(N_TILE - 1, 1)
    base = jax.random.normal(first, shape, jnp.float32)
    rise = jnp.exp(jnp.log(3.0) * position)
    pixel = jnp.exp(jax.random.uniform(second, (F, N_TILE, TH, TW, 1), jnp.float32, -0.5, 0.5))
    channel = jnp.exp(jax.random.uniform(third, (C,), jnp.float32, -1.2, 1.2))
    values = base * rise[None, :, None, None, None] * pixel * channel
    return jnp.clip(values, -8.0, 8.0).astype(jnp.bfloat16)


def block_levels(own_key, shape, shards, low, largest):
    level, own = 1.0, jax.random.fold_in(own_key, 6)
    for dim, parts in shards:
        steps = jnp.exp(jax.random.uniform(jax.random.fold_in(own, dim), (parts,), jnp.float32, low / len(shards), largest / len(shards)))
        level = level * jnp.repeat(steps, shape[dim] // parts).reshape([-1 if axis == dim else 1 for axis in range(len(shape))])
    return level


def scatter_about(own_key, dims, scale, reach, cuts=(), held_as=jnp.bfloat16):
    loudness = block_levels(own_key, dims, cuts, -0.22, 0.18) if cuts else 1.0
    drawn = jax.random.normal(own_key, dims, jnp.float32) * scale * loudness
    return jnp.minimum(jnp.maximum(drawn, -reach), reach).astype(held_as)


def setup_inputs(seed: int = 0, part: int = 0) -> dict:
    key_of = jax.random.split(jax.random.key(seed), 7)
    part_keys = jax.random.split(jax.random.fold_in(key_of[6], part), 7)
    return {
        "frames": draw_frames(jax.random.fold_in(jax.random.fold_in(key_of[6], part), 71), part),
        "cache": scatter_about(part_keys[1], (N_SECTION, CTX, N_TILE, TH, TW, C), 0.6, 4.0, ((0, 4), (2, 64))),
        "conv_weight": scatter_about(key_of[2], (N_SECTION, 3, 3, 3, C, C), (27 * C) ** -0.5, 0.109375, ((0, 4),)),
        "conv_bias": scatter_about(key_of[3], (N_SECTION, C), 0.3, 2.0, ((0, 4),), jnp.float32),
        "norm_gain": jnp.clip(1.0 + 0.18 * jax.random.normal(key_of[4], (N_SECTION, C), jnp.float32), 0.1, 1.9),
        "norm_bias": scatter_about(key_of[5], (N_SECTION, C), 0.3, 2.0, ((0, 4),), jnp.float32),
    }


EPSILON = 1e-06

def to_image(tiles):
    count = tiles.shape[0]
    placed = jnp.roll(tiles, GX + 2, axis=1)
    grid = placed.reshape(count, GY, GX, TH, TW, C)
    return grid.transpose(0, 1, 3, 2, 4, 5).reshape(count, GY * TH, GX * TW, C)

def to_tiles(image):
    count = image.shape[0]
    grid = image.reshape(count, GY, TH, GX, TW, C)
    placed = grid.transpose(0, 1, 3, 2, 4, 5).reshape(count, GY * GX, TH, TW, C)
    return jnp.roll(placed, -(GX + 2), axis=1)

def reference(frames, cache, conv_weight, conv_bias, norm_gain, norm_bias):
    state = to_image(frames)
    height = GY * TH
    width = GX * TW
    results = []
    for section in range(N_SECTION):
        values = state.astype(jnp.float32)
        grouped = values.reshape(F, height * width, GROUPS, C // GROUPS)
        mean = lax.optimization_barrier(jnp.mean(grouped, axis=(1, 3), keepdims=True))
        centered = grouped - mean
        variance = lax.optimization_barrier(jnp.mean(centered * centered, axis=(1, 3), keepdims=True))
        normed = (centered / jnp.sqrt(variance + EPSILON)).reshape(F, height, width, C)
        normed = normed * norm_gain[section] + norm_bias[section]
        active = jax.nn.silu(normed).astype(jnp.bfloat16)
        sequence = jnp.concatenate([to_image(cache[section]), active], axis=0)
        padded = jnp.pad(sequence, ((0, 0), (1, 1), (1, 1), (0, 0)))
        total = jnp.zeros((F * height * width, C), jnp.float32)
        for step_t in range(3):
            for step_y in range(3):
                for step_x in range(3):
                    window = padded[step_t:step_t + F, step_y:step_y + height, step_x:step_x + width]
                    total = total + jnp.dot(window.reshape(F * height * width, C), conv_weight[section, step_t, step_y, step_x], preferred_element_type=jnp.float32)
        total = total.reshape(F, height, width, C)
        state = (values + total + conv_bias[section]).astype(jnp.bfloat16)
        results.append(to_tiles(state))
    return jnp.stack(results)
```

```python
import functools

import jax
import jax.numpy as jnp
from jax import lax
from jax.experimental import pallas as pl
from jax.experimental.pallas import tpu as pltpu
from jax.sharding import PartitionSpec as P

GROUPS = 32
EPSILON = 1e-06
TAPS = 3


def shifted(array, by):
    peers = lax.axis_size("tile")
    return lax.ppermute(array, "tile", [(i, (i + by) % peers) for i in range(peers)])


def summed(array, groups):
    return jnp.sum(lax.all_gather(array, "tile", axis_index_groups=groups), axis=0)


def over_lanes(value, members):
    lanes = value.shape[-1]
    lane = lax.broadcasted_iota(jnp.int32, value.shape, value.ndim - 1)
    step = 1
    while step < members:
        up = pltpu.roll(value, lanes - step, value.ndim - 1)
        down = pltpu.roll(value, step, value.ndim - 1)
        value = value + jnp.where((lane // step) % 2 == 0, up, down)
        step *= 2
    return value


def packed(totals, members):
    totals = over_lanes(totals, members)
    lane = lax.broadcasted_iota(jnp.int32, (1, totals.shape[-1]), 1)
    row = jnp.zeros((1, totals.shape[-1]), jnp.float32)
    for frame in range(totals.shape[0]):
        row = row + jnp.where(lane % members == frame, totals[frame : frame + 1], 0.0)
    return row


def unpacked(row, frame, members):
    lane = lax.broadcasted_iota(jnp.int32, row.shape, 1)
    return over_lanes(jnp.where(lane % members == frame, row, 0.0), members)


def sums_kernel(members, x_ref, sums_ref):
    values = x_ref[...].astype(jnp.float32)
    count = values.shape[0]
    values = values.reshape(count, -1, values.shape[-1])
    sums_ref[0:1, :] = packed(jnp.sum(values, axis=1), members)
    sums_ref[1:2, :] = packed(jnp.sum(values * values, axis=1), members)


def first_sums(frames, members):
    return pl.pallas_call(
        functools.partial(sums_kernel, members),
        out_shape=jax.ShapeDtypeStruct((2, frames.shape[-1]), jnp.float32),
        in_specs=[pl.BlockSpec(memory_space=pltpu.VMEM)],
        out_specs=pl.BlockSpec(memory_space=pltpu.VMEM),
    )(frames)


def section_kernel(
    shape, tick, place_ref, x_ref, sums_ref, cache_ref, kernel_ref, bias_ref, gain_ref, offset_ref,
    kept_ref, next_ref, result_ref, out_sums_ref, act, held, cols, made,
):
    count, context, side, wide, sections, pixels, members = shape
    rows_in = wide - 2 * tick
    rows_out = rows_in - 2
    channels = x_ref.shape[-1]
    flat_in = rows_in * wide
    flat_out = rows_out * wide
    first_row, last_row, first_col, last_col, mine = (place_ref[i] for i in range(5))

    def inside(edge, rows):
        row = lax.broadcasted_iota(jnp.int32, (rows, wide, channels), 0)
        col = lax.broadcasted_iota(jnp.int32, (rows, wide, channels), 1)
        far = edge + side
        low_r = jnp.where(first_row == 1, edge, 0)
        high_r = jnp.where(last_row == 1, far, far + edge)
        low_c = jnp.where(first_col == 1, edge, 0)
        high_c = jnp.where(last_col == 1, far, far + edge)
        return (row >= low_r) & (row < high_r) & (col >= low_c) & (col < high_c)

    halo = (wide - side) // 2
    valid = inside(halo, wide)
    for f in range(context):
        values = cache_ref[f].astype(jnp.float32).reshape(wide, wide, channels)
        act[f, : wide * wide] = jnp.where(valid, values, 0.0).reshape(wide * wide, channels)
    total = jnp.sum(sums_ref[...], axis=0)
    mean_row = total[0:1] / pixels
    square_row = total[1:2] / pixels
    valid = inside(halo - tick, rows_in)
    gain = gain_ref[...].reshape(1, channels)
    offset = offset_ref[...].reshape(1, channels)
    for f in range(count):
        mean = unpacked(mean_row, f, members)
        variance = jnp.maximum(unpacked(square_row, f, members) - mean * mean, 0.0)
        scale = gain / jnp.sqrt(variance + EPSILON)
        values = x_ref[f].astype(jnp.float32)
        held[f, :flat_in] = values
        normed = (values - mean) * scale + offset
        half = 0.5 * normed
        active = (half + half * jnp.tanh(half)).reshape(rows_in, wide, channels)
        active = jnp.where(valid, active, 0.0).reshape(flat_in, channels)
        act[context + f, :flat_in] = active
    for f in range(context + count):
        base = tick * (wide + 1) if f < context else 0
        for dy in range(TAPS):
            for dx in range(TAPS):
                at = base + dy * wide + dx
                piece = act[f, at : at + flat_out].astype(jnp.bfloat16)
                tap = (dy * TAPS + dx) * channels
                cols[f, :flat_out, tap : tap + channels] = piece
    w0, w1, w2 = (kernel_ref[i] for i in range(TAPS))
    both_1 = jnp.concatenate([w1, w0], axis=1)
    both_2 = jnp.concatenate([w2, w1], axis=1)
    bias = bias_ref[...].reshape(1, channels)

    def dot(f, weights):
        return jnp.dot(cols[f, :flat_out], weights, preferred_element_type=jnp.float32)

    for f in range(0, count, 2):
        pair = dot(f + 1, both_1) + dot(f + 2, both_2)
        first = pair[:, :channels] + dot(f, w0)
        second = pair[:, channels:] + dot(f + 3, w2)
        for g, value in ((f, first), (f + 1, second)):
            new = value + bias + held[g, wide + 1 : wide + 1 + flat_out]
            made[g, :flat_out] = new.astype(jnp.bfloat16).astype(jnp.float32)
    edge = halo - tick - 1
    sums, squares = [], []
    for f in range(count):
        if next_ref is not None:
            next_ref[f] = made[f, :flat_out].astype(jnp.bfloat16)
        total_f = jnp.zeros((1, channels), jnp.float32)
        square_f = jnp.zeros((1, channels), jnp.float32)
        for y in range(side):
            at = (y + edge) * wide + edge
            row = made[f, at : at + side]
            if out_sums_ref is not None:
                total_f = total_f + jnp.sum(row, axis=0, keepdims=True)
                square_f = square_f + jnp.sum(row * row, axis=0, keepdims=True)
            row = row.astype(jnp.bfloat16)
            if kept_ref is not None:
                row = jnp.where(mine == 1, row, kept_ref[f, y])
            result_ref[f, y] = row
        sums.append(total_f)
        squares.append(square_f)
    if out_sums_ref is not None:
        out_sums_ref[0:1, :] = packed(jnp.concatenate(sums, axis=0), members)
        out_sums_ref[1:2, :] = packed(jnp.concatenate(squares, axis=0), members)


def section_step(shape, tick, place, x, sums, cache, kernel, bias, gain, offset, kept):
    count, context, side, wide, sections, pixels, members = shape
    channels = x.shape[-1]
    rows_out = wide - 2 * tick - 2
    last = tick == sections - 1
    vmem = pl.BlockSpec(memory_space=pltpu.VMEM)
    inputs = [place, x, sums, cache, kernel, bias, gain, offset]
    if kept is not None:
        inputs.append(kept)
    outs = [jax.ShapeDtypeStruct((count, side, side, channels), jnp.bfloat16)]
    if not last:
        outs.insert(0, jax.ShapeDtypeStruct((count, rows_out * wide, channels), jnp.bfloat16))
        outs.append(jax.ShapeDtypeStruct((2, channels), jnp.float32))

    def body(*refs):
        refs = list(refs)
        given = refs[:8]
        del refs[:8]
        kept_ref = refs.pop(0) if kept is not None else None
        next_ref = refs.pop(0) if not last else None
        result_ref = refs.pop(0)
        out_sums_ref = refs.pop(0) if not last else None
        section_kernel(shape, tick, *given, kept_ref, next_ref, result_ref, out_sums_ref, *refs)

    full = wide * wide + 8
    return pl.pallas_call(
        body,
        out_shape=tuple(outs),
        in_specs=[pl.BlockSpec(memory_space=pltpu.SMEM)] + [vmem] * (len(inputs) - 1),
        out_specs=tuple([vmem] * len(outs)),
        scratch_shapes=[
            pltpu.VMEM((context + count, full, channels), jnp.float32),
            pltpu.VMEM((count, full, channels), jnp.float32),
            pltpu.VMEM((context + count, rows_out * wide, TAPS * TAPS * channels), jnp.bfloat16),
            pltpu.VMEM((count, rows_out * wide, channels), jnp.float32),
        ],
        name=f"section_{tick}",
    )(*inputs)


def local(frames, cache, conv_weight, conv_bias, norm_gain, norm_bias):
    sections = lax.axis_size("section")
    tiles = lax.axis_size("tile")
    across = min(8, tiles // 2)
    down = tiles // across
    position = lax.axis_index("section")
    placed = (lax.axis_index("tile") + across + 2) % tiles
    column, row_at = placed % across, placed // across
    x = frames[:, 0]
    count, side, _, channels = x.shape
    members = channels // GROUPS
    halo = sections
    wide = side + 2 * halo
    pixels = float(side * side * members * tiles)
    shape = (count, cache.shape[1], side, wide, sections, pixels, members)
    near = [[across * g + j for j in range(across)] for g in range(down)]
    far = [[g + across * j for j in range(down)] for g in range(across)]

    seq = jnp.concatenate([cache[0, :, 0], x], axis=0)
    left = shifted(seq[:, :, side - halo :], 1)
    right = shifted(seq[:, :, :halo], -1)
    sums = summed(first_sums(x, members), near)
    seq = jnp.concatenate([left, seq, right], axis=2)
    above = shifted(seq[:, side - halo :], across)
    below = shifted(seq[:, :halo], -across)
    sums = lax.all_gather(sums, "tile", axis_index_groups=far)
    seq = jnp.concatenate([above, seq, below], axis=1).reshape(seq.shape[0], wide * wide, channels)
    held_cache, x = seq[: cache.shape[1]], seq[cache.shape[1] :]

    flags = [row_at == 0, row_at == down - 1, column == 0, column == across - 1]
    kernel = conv_weight[0].reshape(TAPS, TAPS * TAPS * channels, channels)
    result = None
    for tick in range(sections):
        place = jnp.stack(flags + [position == tick]).astype(jnp.int32)
        made = section_step(
            shape, tick, place, x, sums, held_cache, kernel, conv_bias, norm_gain, norm_bias, result
        )
        if tick + 1 == sections:
            (result,) = made
            break
        x, result, sums = made
        hop = [(tick, tick + 1)]
        sums = lax.ppermute(sums, "section", hop)
        x = lax.ppermute(x, "section", hop)
        sums = summed(sums, near)
        sums = lax.all_gather(sums, "tile", axis_index_groups=far)
    return result[None, :, None]


def solution(mesh):
    placed = (
        P("parts", "tile", None, None, None),
        P("section", "parts", "tile", None, None, None),
        P("section", None, None, None, None, None),
        P("section", None),
        P("section", None),
        P("section", None),
    )
    return jax.shard_map(
        local,
        mesh=mesh,
        in_specs=placed,
        out_specs=P("section", "parts", "tile", None, None, None),
        check_vma=False,
    )
```

```python
import functools

import jax
import jax.numpy as jnp
from jax import lax
from jax.experimental import pallas as pl
from jax.experimental.pallas import tpu as pltpu
from jax.sharding import PartitionSpec as P

GROUPS = 32
EPSILON = 1e-06
TAPS = 3
VMEM_LIMIT = 20 * 1024 * 1024


def shifted(array, by):
    peers = lax.axis_size("tile")
    return lax.ppermute(array, "tile", [(i, (i + by) % peers) for i in range(peers)])


def of_everyone(sums):
    peers = lax.axis_size("tile")
    copies = jnp.broadcast_to(sums.reshape(1, 1, sums.size), (peers, 1, sums.size))
    return jnp.sum(lax.all_to_all(copies, "tile", 0, 0, tiled=True), axis=0).reshape(sums.shape)


def over_lanes(value, members):
    lanes = value.shape[-1]
    lane = lax.broadcasted_iota(jnp.int32, value.shape, value.ndim - 1)
    step = 1
    while step < members:
        up = pltpu.roll(value, lanes - step, value.ndim - 1)
        down = pltpu.roll(value, step, value.ndim - 1)
        value = value + jnp.where((lane // step) % 2 == 0, up, down)
        step *= 2
    return value


def packed(totals, members):
    totals = over_lanes(totals, members)
    lane = lax.broadcasted_iota(jnp.int32, (1, totals.shape[-1]), 1)
    row = jnp.zeros((1, totals.shape[-1]), jnp.float32)
    for frame in range(totals.shape[0]):
        row = row + jnp.where(lane % members == frame, totals[frame : frame + 1], 0.0)
    return row


def unpacked(row, frame, members):
    lane = lax.broadcasted_iota(jnp.int32, row.shape, 1)
    return over_lanes(jnp.where(lane % members == frame, row, 0.0), members)


def sums_kernel(members, x_ref, sums_ref):
    values = x_ref[...].astype(jnp.float32)
    count = values.shape[0]
    values = values.reshape(count, -1, values.shape[-1])
    sums_ref[0:1, :] = packed(jnp.sum(values, axis=1), members)
    sums_ref[1:2, :] = packed(jnp.sum(values * values, axis=1), members)


def first_sums(frames, members):
    return pl.pallas_call(
        functools.partial(sums_kernel, members),
        out_shape=jax.ShapeDtypeStruct((2, frames.shape[-1]), jnp.float32),
        in_specs=[pl.BlockSpec(memory_space=pltpu.VMEM)],
        out_specs=pl.BlockSpec(memory_space=pltpu.VMEM),
    )(frames)


def masked(flags, edge, rows, wide, side, channels):
    first_row, last_row, first_col, last_col = flags
    row = lax.broadcasted_iota(jnp.int32, (rows, wide, channels), 0)
    col = lax.broadcasted_iota(jnp.int32, (rows, wide, channels), 1)
    far = edge + side
    low_r = jnp.where(first_row == 1, edge, 0)
    high_r = jnp.where(last_row == 1, far, far + edge)
    low_c = jnp.where(first_col == 1, edge, 0)
    high_c = jnp.where(last_col == 1, far, far + edge)
    return (row >= low_r) & (row < high_r) & (col >= low_c) & (col < high_c)


def unfold(act, cols, frame, wide, rows, channels):
    for dy in range(TAPS):
        for dx in range(TAPS):
            at = dy * wide + dx
            tap = (dy * TAPS + dx) * channels
            cols[frame, :rows, tap : tap + channels] = act[frame, at : at + rows].astype(jnp.bfloat16)


def matmul(cols, frame, rows, weights):
    return jnp.dot(cols[frame, :rows], weights, preferred_element_type=jnp.float32)


def context_kernel(side, wide, place_ref, cache_ref, kernel_ref, bias_ref, part_ref, act, cols):
    context = cache_ref.shape[0]
    channels = cache_ref.shape[-1]
    flags = [place_ref[i] for i in range(4)]
    valid = masked(flags, (wide - side) // 2, wide, wide, side, channels)
    rows = (wide - 2) * wide
    for f in range(context):
        values = cache_ref[f].astype(jnp.float32).reshape(wide, wide, channels)
        act[f, : wide * wide] = jnp.where(valid, values, 0.0).reshape(wide * wide, channels)
        act[f, wide * wide :] = jnp.zeros((act.shape[1] - wide * wide, channels), jnp.float32)
        unfold(act, cols, f, wide, rows, channels)
    w0, w1 = kernel_ref[0], kernel_ref[1]
    bias = bias_ref[...].reshape(1, channels)
    pair = matmul(cols, 1, rows, jnp.concatenate([w1, w0], axis=1))
    part_ref[0] = pair[:, :channels] + matmul(cols, 0, rows, w0) + bias
    part_ref[1] = pair[:, channels:] + bias


def context_part(side, wide, place, cache, kernel, bias):
    channels = cache.shape[-1]
    vmem = pl.BlockSpec(memory_space=pltpu.VMEM)
    rows = (wide - 2) * wide
    return pl.pallas_call(
        functools.partial(context_kernel, side, wide),
        out_shape=jax.ShapeDtypeStruct((2, rows, channels), jnp.float32),
        in_specs=[pl.BlockSpec(memory_space=pltpu.SMEM), vmem, vmem, vmem],
        out_specs=vmem,
        scratch_shapes=[
            pltpu.VMEM((cache.shape[0], wide * wide + 8, channels), jnp.float32),
            pltpu.VMEM((cache.shape[0], rows, TAPS * TAPS * channels), jnp.bfloat16),
        ],
        compiler_params=pltpu.CompilerParams(vmem_limit_bytes=VMEM_LIMIT),
        name="context",
    )(place, cache, kernel, bias)


def section_kernel(
    shape, tick, place_ref, x_ref, sums_ref, part_ref, kernel_ref, bias_ref, gain_ref, offset_ref,
    kept_ref, next_ref, result_ref, out_sums_ref, act, held, cols, made,
):
    count, side, wide, sections, pixels, members = shape
    rows_in = wide - 2 * tick
    rows_out = rows_in - 2
    channels = x_ref.shape[-1]
    flat_in = rows_in * wide
    flat_out = rows_out * wide
    halo = (wide - side) // 2
    flags = [place_ref[i] for i in range(4)]
    position = place_ref[4]
    mean_row = sums_ref[0:1] / pixels
    square_row = sums_ref[1:2] / pixels
    valid = masked(flags, halo - tick, rows_in, wide, side, channels)
    gain = gain_ref[...].reshape(1, channels)
    offset = offset_ref[...].reshape(1, channels)
    for f in range(count):
        mean = unpacked(mean_row, f, members)
        variance = jnp.maximum(unpacked(square_row, f, members) - mean * mean, 0.0)
        scale = gain / jnp.sqrt(variance + EPSILON)
        values = x_ref[f].astype(jnp.float32)
        held[f, :flat_in] = values
        normed = (values - mean) * scale + offset
        half = 0.5 * normed
        active = (half + half * jnp.tanh(half)).reshape(rows_in, wide, channels)
        active = jnp.where(valid, active, 0.0).reshape(flat_in, channels)
        act[f, :flat_in] = active
        unfold(act, cols, f, wide, flat_out, channels)
    w0, w1, w2 = (kernel_ref[i] for i in range(TAPS))
    both_1 = jnp.concatenate([w1, w0], axis=1)
    both_2 = jnp.concatenate([w2, w1], axis=1)
    bias = bias_ref[...].reshape(1, channels)
    base = tick * (wide + 1)

    def finish(g, value):
        new = value + held[g, wide + 1 : wide + 1 + flat_out]
        made[g, :flat_out] = new.astype(jnp.bfloat16).astype(jnp.float32)

    for f in range(0, count, 2):
        pair = matmul(cols, f, flat_out, both_2)
        first = pair[:, :channels]
        second = pair[:, channels:] + matmul(cols, f + 1, flat_out, w2)
        if f == 0:
            finish(f, first + part_ref[0, base : base + flat_out])
            finish(f + 1, second + part_ref[1, base : base + flat_out])
        else:
            pair = matmul(cols, f - 1, flat_out, both_1)
            first = first + pair[:, :channels] + matmul(cols, f - 2, flat_out, w0)
            finish(f, first + bias)
            finish(f + 1, second + pair[:, channels:] + bias)
    edge = halo - tick - 1
    sums, squares = [], []
    for f in range(count):
        if next_ref is not None:
            next_ref[f] = made[f, :flat_out].astype(jnp.bfloat16)
        total_f = jnp.zeros((side, channels), jnp.float32)
        square_f = jnp.zeros((side, channels), jnp.float32)
        for y in range(side):
            at = (y + edge) * wide + edge
            row = made[f, at : at + side]
            if out_sums_ref is not None:
                total_f = total_f + row
                square_f = square_f + row * row
            row = row.astype(jnp.bfloat16)
            if kept_ref is not None:
                row = jnp.where(position == tick, row, kept_ref[f, y])
            result_ref[f, y] = row
        sums.append(jnp.sum(total_f, axis=0, keepdims=True))
        squares.append(jnp.sum(square_f, axis=0, keepdims=True))
    if out_sums_ref is not None:
        out_sums_ref[0:1, :] = packed(jnp.concatenate(sums, axis=0), members)
        out_sums_ref[1:2, :] = packed(jnp.concatenate(squares, axis=0), members)


def section_step(shape, tick, place, x, sums, part, kernel, bias, gain, offset, kept):
    count, side, wide, sections, pixels, members = shape
    channels = x.shape[-1]
    rows_out = wide - 2 * tick - 2
    last = tick == sections - 1
    vmem = pl.BlockSpec(memory_space=pltpu.VMEM)
    inputs = [place, x, sums, part, kernel, bias, gain, offset]
    if kept is not None:
        inputs.append(kept)
    outs = [jax.ShapeDtypeStruct((count, side, side, channels), jnp.bfloat16)]
    if not last:
        outs.insert(0, jax.ShapeDtypeStruct((count, rows_out * wide, channels), jnp.bfloat16))
        outs.append(jax.ShapeDtypeStruct((2, channels), jnp.float32))

    def body(*refs):
        refs = list(refs)
        given = refs[:8]
        del refs[:8]
        kept_ref = refs.pop(0) if kept is not None else None
        next_ref = refs.pop(0) if not last else None
        result_ref = refs.pop(0)
        out_sums_ref = refs.pop(0) if not last else None
        section_kernel(shape, tick, *given, kept_ref, next_ref, result_ref, out_sums_ref, *refs)

    full = wide * wide + 8
    return pl.pallas_call(
        body,
        out_shape=tuple(outs),
        in_specs=[pl.BlockSpec(memory_space=pltpu.SMEM)] + [vmem] * (len(inputs) - 1),
        out_specs=tuple([vmem] * len(outs)),
        scratch_shapes=[
            pltpu.VMEM((count, full, channels), jnp.float32),
            pltpu.VMEM((count, full, channels), jnp.float32),
            pltpu.VMEM((count, rows_out * wide, TAPS * TAPS * channels), jnp.bfloat16),
            pltpu.VMEM((count, rows_out * wide, channels), jnp.float32),
        ],
        compiler_params=pltpu.CompilerParams(vmem_limit_bytes=VMEM_LIMIT),
        name=f"section_{tick}",
    )(*inputs)


def local(frames, cache, conv_weight, conv_bias, norm_gain, norm_bias):
    sections = lax.axis_size("section")
    tiles = lax.axis_size("tile")
    across = min(8, tiles // 2)
    down = tiles // across
    position = lax.axis_index("section")
    placed = (lax.axis_index("tile") + across + 2) % tiles
    column, row_at = placed % across, placed // across
    x = frames[:, 0]
    count, side, _, channels = x.shape
    members = channels // GROUPS
    halo = sections
    wide = side + 2 * halo
    pixels = float(side * side * members * tiles)
    shape = (count, side, wide, sections, pixels, members)
    flags = [row_at == 0, row_at == down - 1, column == 0, column == across - 1]
    place = jnp.stack([f.astype(jnp.int32) for f in flags] + [position.astype(jnp.int32)])
    kernel = conv_weight[0].reshape(TAPS, TAPS * TAPS * channels, channels)

    old = cache[0, :, 0]
    sums = first_sums(x, members)
    sums, seq = lax.optimization_barrier((sums, jnp.concatenate([old, x], axis=0)))
    sums = of_everyone(sums)
    left = shifted(seq[:, :, side - halo :], 1)
    right = shifted(seq[:, :, :halo], -1)
    middle = jnp.concatenate([left, seq, right], axis=2)
    above = shifted(middle[:, side - halo :], across)
    below = shifted(middle[:, :halo], -across)
    whole = jnp.concatenate([above, middle, below], axis=1)
    whole = whole.reshape(whole.shape[0], wide * wide, channels)
    context = old.shape[0]
    x = whole[context:]
    part = context_part(side, wide, place, whole[:context], kernel, conv_bias)

    result = None
    for tick in range(sections):
        made = section_step(
            shape, tick, place, x, sums, part, kernel, conv_bias, norm_gain, norm_bias, result
        )
        if tick + 1 == sections:
            (result,) = made
            break
        x, result, sums = made
        hop = [(tick, tick + 1)]
        sums = lax.ppermute(sums, "section", hop)
        sums, x = lax.optimization_barrier((sums, x))
        sums = of_everyone(sums)
        x = lax.ppermute(x, "section", hop)
    return result[None, :, None]


def solution(mesh):
    placed = (
        P("parts", "tile", None, None, None),
        P("section", "parts", "tile", None, None, None),
        P("section", None, None, None, None, None),
        P("section", None),
        P("section", None),
        P("section", None),
    )
    return jax.shard_map(
        local,
        mesh=mesh,
        in_specs=placed,
        out_specs=P("section", "parts", "tile", None, None, None),
        check_vma=False,
    )
```

```python
import functools

import jax
import jax.numpy as jnp
from jax import lax
from jax.experimental import pallas as pl
from jax.experimental.pallas import tpu as pltpu
from jax.sharding import PartitionSpec as P


GROUPS = 32
EPSILON = 1e-06
TAPS = 3
VMEM_LIMIT = 20 * 1024 * 1024


def shifted(array, by):
    peers = lax.axis_size("tile")
    return lax.ppermute(array, "tile", [(i, (i + by) % peers) for i in range(peers)])


def of_everyone(sums):
    peers = lax.axis_size("tile")
    copies = jnp.broadcast_to(sums.reshape(1, 1, sums.size), (peers, 1, sums.size))
    return jnp.sum(lax.all_to_all(copies, "tile", 0, 0, tiled=True), axis=0).reshape(sums.shape)


def over_lanes(value, members):
    lanes = value.shape[-1]
    lane = lax.broadcasted_iota(jnp.int32, value.shape, value.ndim - 1)
    step = 1
    while step < members:
        up = pltpu.roll(value, lanes - step, value.ndim - 1)
        down = pltpu.roll(value, step, value.ndim - 1)
        value = value + jnp.where((lane // step) % 2 == 0, up, down)
        step *= 2
    return value


def packed(totals, members):
    totals = over_lanes(totals, members)
    lane = lax.broadcasted_iota(jnp.int32, (1, totals.shape[-1]), 1)
    row = jnp.zeros((1, totals.shape[-1]), jnp.float32)
    for frame in range(totals.shape[0]):
        row = row + jnp.where(lane % members == frame, totals[frame : frame + 1], 0.0)
    return row


def unpacked(row, frame, members):
    lane = lax.broadcasted_iota(jnp.int32, row.shape, 1)
    return over_lanes(jnp.where(lane % members == frame, row, 0.0), members)


def sums_kernel(members, x_ref, sums_ref):
    values = x_ref[...].astype(jnp.float32)
    count = values.shape[0]
    values = values.reshape(count, -1, values.shape[-1])
    sums_ref[0:1, :] = packed(jnp.sum(values, axis=1), members)
    sums_ref[1:2, :] = packed(jnp.sum(values * values, axis=1), members)


def first_sums(frames, members):
    return pl.pallas_call(
        functools.partial(sums_kernel, members),
        out_shape=jax.ShapeDtypeStruct((2, frames.shape[-1]), jnp.float32),
        in_specs=[pl.BlockSpec(memory_space=pltpu.VMEM)],
        out_specs=pl.BlockSpec(memory_space=pltpu.VMEM),
    )(frames)


def masked(flags, edge, rows, wide, side, channels):
    first_row, last_row, first_col, last_col = flags
    row = lax.broadcasted_iota(jnp.int32, (rows, wide, channels), 0)
    col = lax.broadcasted_iota(jnp.int32, (rows, wide, channels), 1)
    far = edge + side
    low_r = jnp.where(first_row == 1, edge, 0)
    high_r = jnp.where(last_row == 1, far, far + edge)
    low_c = jnp.where(first_col == 1, edge, 0)
    high_c = jnp.where(last_col == 1, far, far + edge)
    return (row >= low_r) & (row < high_r) & (col >= low_c) & (col < high_c)


def unfold(act, cols, frame, wide, rows, channels):
    for dy in range(TAPS):
        for dx in range(TAPS):
            at = dy * wide + dx
            tap = (dy * TAPS + dx) * channels
            cols[frame, :rows, tap : tap + channels] = act[frame, at : at + rows].astype(jnp.bfloat16)


def matmul(cols, frame, rows, weights):
    return jnp.dot(cols[frame, :rows], weights, preferred_element_type=jnp.float32)


def context_kernel(side, wide, place_ref, cache_ref, kernel_hbm, bias_ref, part_ref, act, cols, kernel_ref, sem):
    fetch = pltpu.make_async_copy(kernel_hbm.at[:2], kernel_ref, sem)
    fetch.start()
    context = cache_ref.shape[0]
    channels = cache_ref.shape[-1]
    flags = [place_ref[i] for i in range(4)]
    valid = masked(flags, (wide - side) // 2, wide, wide, side, channels)
    rows = (wide - 2) * wide
    for f in range(context):
        values = cache_ref[f].astype(jnp.float32).reshape(wide, wide, channels)
        act[f, : wide * wide] = jnp.where(valid, values, 0.0).reshape(wide * wide, channels)
        act[f, wide * wide :] = jnp.zeros((act.shape[1] - wide * wide, channels), jnp.float32)
        unfold(act, cols, f, wide, rows, channels)
    fetch.wait()
    w0, w1 = kernel_ref[0], kernel_ref[1]
    bias = bias_ref[...].reshape(1, channels)
    pair = matmul(cols, 1, rows, jnp.concatenate([w1, w0], axis=1))
    part_ref[0] = pair[:, :channels] + matmul(cols, 0, rows, w0) + bias
    part_ref[1] = pair[:, channels:] + bias


def context_part(side, wide, place, cache, kernel, bias):
    channels = cache.shape[-1]
    vmem = pl.BlockSpec(memory_space=pltpu.VMEM)
    rows = (wide - 2) * wide
    return pl.pallas_call(
        functools.partial(context_kernel, side, wide),
        out_shape=jax.ShapeDtypeStruct((2, rows, channels), jnp.float32),
        in_specs=[pl.BlockSpec(memory_space=pltpu.SMEM), vmem, pl.BlockSpec(memory_space=pltpu.HBM), vmem],
        out_specs=vmem,
        scratch_shapes=[
            pltpu.VMEM((cache.shape[0], wide * wide + 8, channels), jnp.float32),
            pltpu.VMEM((cache.shape[0], rows, TAPS * TAPS * channels), jnp.bfloat16),
            pltpu.VMEM((2, *kernel.shape[1:]), kernel.dtype),
            pltpu.SemaphoreType.DMA,
        ],
        compiler_params=pltpu.CompilerParams(vmem_limit_bytes=VMEM_LIMIT),
        name="context",
    )(place, cache, kernel, bias)


def section_kernel(
    shape, tick, place_ref, x_ref, sums_ref, part_ref, kernel_hbm, bias_ref, gain_ref, offset_ref,
    kept_ref, next_ref, result_ref, out_sums_ref, act, held, cols, made, kernel_ref, sem,
):
    fetch = pltpu.make_async_copy(kernel_hbm, kernel_ref, sem)
    fetch.start()
    count, side, wide, _, pixels, members = shape
    rows_in = wide - 2 * tick
    rows_out = rows_in - 2
    channels = x_ref.shape[-1]
    flat_in = rows_in * wide
    flat_out = rows_out * wide
    halo = (wide - side) // 2
    flags = [place_ref[i] for i in range(4)]
    position = place_ref[4]
    mean_row = sums_ref[0:1] / pixels
    square_row = sums_ref[1:2] / pixels
    valid = masked(flags, halo - tick, rows_in, wide, side, channels)
    gain = gain_ref[...].reshape(1, channels)
    offset = offset_ref[...].reshape(1, channels)
    for f in range(count):
        mean = unpacked(mean_row, f, members)
        variance = jnp.maximum(unpacked(square_row, f, members) - mean * mean, 0.0)
        scale = gain / jnp.sqrt(variance + EPSILON)
        values = x_ref[f].astype(jnp.float32)
        held[f, :flat_in] = values
        normed = (values - mean) * scale + offset
        half = 0.5 * normed
        active = (half + half * jnp.tanh(half)).reshape(rows_in, wide, channels)
        active = jnp.where(valid, active, 0.0).reshape(flat_in, channels)
        act[f, :flat_in] = active
        unfold(act, cols, f, wide, flat_out, channels)
    fetch.wait()
    w0, w1, w2 = (kernel_ref[i] for i in range(TAPS))
    both_1 = jnp.concatenate([w1, w0], axis=1)
    both_2 = jnp.concatenate([w2, w1], axis=1)
    bias = bias_ref[...].reshape(1, channels)
    base = tick * (wide + 1)

    def finish(g, value):
        new = value + held[g, wide + 1 : wide + 1 + flat_out]
        made[g, :flat_out] = new.astype(jnp.bfloat16).astype(jnp.float32)

    for f in range(0, count, 2):
        pair = matmul(cols, f, flat_out, both_2)
        first = pair[:, :channels]
        second = pair[:, channels:] + matmul(cols, f + 1, flat_out, w2)
        if f == 0:
            finish(f, first + part_ref[0, base : base + flat_out])
            finish(f + 1, second + part_ref[1, base : base + flat_out])
        else:
            pair = matmul(cols, f - 1, flat_out, both_1)
            first = first + pair[:, :channels] + matmul(cols, f - 2, flat_out, w0)
            finish(f, first + bias)
            finish(f + 1, second + pair[:, channels:] + bias)
    edge = halo - tick - 1
    sums, squares = [], []
    for f in range(count):
        if next_ref is not None:
            next_ref[f] = made[f, :flat_out].astype(jnp.bfloat16)
        total_f = jnp.zeros((side, channels), jnp.float32)
        square_f = jnp.zeros((side, channels), jnp.float32)
        for y in range(side):
            at = (y + edge) * wide + edge
            row = made[f, at : at + side]
            if out_sums_ref is not None:
                total_f = total_f + row
                square_f = square_f + row * row
            row = row.astype(jnp.bfloat16)
            if kept_ref is not None:
                row = jnp.where(position == tick, row, kept_ref[f, y])
            result_ref[f, y] = row
        sums.append(jnp.sum(total_f, axis=0, keepdims=True))
        squares.append(jnp.sum(square_f, axis=0, keepdims=True))
    if out_sums_ref is not None:
        out_sums_ref[0:1, :] = packed(jnp.concatenate(sums, axis=0), members)
        out_sums_ref[1:2, :] = packed(jnp.concatenate(squares, axis=0), members)


def section_step(shape, tick, place, x, sums, part, kernel, bias, gain, offset, kept):
    count, side, wide, sections, _, _ = shape
    channels = x.shape[-1]
    rows_out = wide - 2 * tick - 2
    last = tick == sections - 1
    vmem = pl.BlockSpec(memory_space=pltpu.VMEM)
    inputs = [place, x, sums, part, kernel, bias, gain, offset]
    if kept is not None:
        inputs.append(kept)
    outs = [jax.ShapeDtypeStruct((count, side, side, channels), jnp.bfloat16)]
    if not last:
        outs.insert(0, jax.ShapeDtypeStruct((count, rows_out * wide, channels), jnp.bfloat16))
        outs.append(jax.ShapeDtypeStruct((2, channels), jnp.float32))

    def body(*refs):
        refs = list(refs)
        given = refs[:8]
        del refs[:8]
        kept_ref = refs.pop(0) if kept is not None else None
        next_ref = refs.pop(0) if not last else None
        result_ref = refs.pop(0)
        out_sums_ref = refs.pop(0) if not last else None
        section_kernel(shape, tick, *given, kept_ref, next_ref, result_ref, out_sums_ref, *refs)

    full = wide * wide + 8
    return pl.pallas_call(
        body,
        out_shape=tuple(outs),
        in_specs=[pl.BlockSpec(memory_space=pltpu.SMEM), vmem, vmem, vmem, pl.BlockSpec(memory_space=pltpu.HBM)]
        + [vmem] * (len(inputs) - 5),
        out_specs=tuple([vmem] * len(outs)),
        scratch_shapes=[
            pltpu.VMEM((count, full, channels), jnp.float32),
            pltpu.VMEM((count, full, channels), jnp.float32),
            pltpu.VMEM((count, rows_out * wide, TAPS * TAPS * channels), jnp.bfloat16),
            pltpu.VMEM((count, rows_out * wide, channels), jnp.float32),
            pltpu.VMEM(kernel.shape, kernel.dtype),
            pltpu.SemaphoreType.DMA,
        ],
        compiler_params=pltpu.CompilerParams(vmem_limit_bytes=VMEM_LIMIT),
    )(*inputs)


def local(frames, cache, conv_weight, conv_bias, norm_gain, norm_bias):
    sections = lax.axis_size("section")
    tiles = lax.axis_size("tile")
    across = min(8, tiles // 2)
    down = tiles // across
    position = lax.axis_index("section")
    placed = (lax.axis_index("tile") + across + 2) % tiles
    column, row_at = placed % across, placed // across
    x = frames[:, 0]
    count, side, _, channels = x.shape
    members = channels // GROUPS
    halo = sections
    wide = side + 2 * halo
    pixels = float(side * side * members * tiles)
    shape = (count, side, wide, sections, pixels, members)
    flags = [row_at == 0, row_at == down - 1, column == 0, column == across - 1]
    place = jnp.stack([f.astype(jnp.int32) for f in flags] + [position.astype(jnp.int32)])
    kernel = conv_weight[0].reshape(TAPS, TAPS * TAPS * channels, channels)

    old = cache[0, :, 0]
    context = old.shape[0]
    sums = first_sums(x, members)
    seq = jnp.concatenate([old, x], axis=0)
    left = shifted(seq[:, :, side - halo :], 1)
    right = shifted(seq[:, :, :halo], -1)
    middle = jnp.concatenate([left, seq, right], axis=2)
    above = shifted(middle[:, side - halo :], across)
    below = shifted(middle[:, :halo], -across)
    sums = of_everyone(sums)
    held_cache, x = (
        jnp.concatenate([above[c], middle[c], below[c]], axis=1).reshape(-1, wide * wide, channels)
        for c in (slice(0, context), slice(context, None))
    )
    part = context_part(side, wide, place, held_cache, kernel, conv_bias)

    result = None
    for tick in range(sections):
        made = section_step(
            shape, tick, place, x, sums, part, kernel, conv_bias, norm_gain, norm_bias, result
        )
        if tick + 1 == sections:
            (result,) = made
            break
        x, result, sums = made
        hop = [(tick, tick + 1)]
        sums = lax.ppermute(sums, "section", hop)
        sums, x = lax.optimization_barrier((sums, x))
        x = lax.ppermute(x, "section", hop)
        sums = of_everyone(sums)
    return result[None, :, None]


def solution(mesh):
    placed = (
        P("parts", "tile", None, None, None),
        P("section", "parts", "tile", None, None, None),
        P("section", None, None, None, None, None),
        P("section", None),
        P("section", None),
        P("section", None),
    )
    return jax.shard_map(
        local,
        mesh=mesh,
        in_specs=placed,
        out_specs=P("section", "parts", "tile", None, None, None),
        check_vma=False,
    )
```

```python
import functools

import jax
import jax.numpy as jnp
from jax import lax
from jax.experimental import pallas as pl
from jax.experimental.pallas import tpu as pltpu
from jax.sharding import PartitionSpec as P


GROUPS = 32
EPSILON = 1e-06
TAPS = 3
VMEM_LIMIT = 20 * 1024 * 1024


def shifted(array, by):
    peers = lax.axis_size("tile")
    return lax.ppermute(array, "tile", [(i, (i + by) % peers) for i in range(peers)])


def of_everyone(sums):
    peers = lax.axis_size("tile")
    copies = jnp.broadcast_to(sums.reshape(1, 1, sums.size), (peers, 1, sums.size))
    return jnp.sum(lax.all_to_all(copies, "tile", 0, 0, tiled=True), axis=0).reshape(sums.shape)


def over_lanes(value, members):
    lanes = value.shape[-1]
    lane = lax.broadcasted_iota(jnp.int32, value.shape, value.ndim - 1)
    step = 1
    while step < members:
        up = pltpu.roll(value, lanes - step, value.ndim - 1)
        down = pltpu.roll(value, step, value.ndim - 1)
        value = value + jnp.where((lane // step) % 2 == 0, up, down)
        step *= 2
    return value


def packed(totals, members):
    totals = over_lanes(totals, members)
    lane = lax.broadcasted_iota(jnp.int32, (1, totals.shape[-1]), 1)
    row = jnp.zeros((1, totals.shape[-1]), jnp.float32)
    for frame in range(totals.shape[0]):
        row = row + jnp.where(lane % members == frame, totals[frame : frame + 1], 0.0)
    return row


def unpacked(row, frame, members):
    lane = lax.broadcasted_iota(jnp.int32, row.shape, 1)
    return over_lanes(jnp.where(lane % members == frame, row, 0.0), members)


def sums_kernel(members, x_ref, sums_ref):
    values = x_ref[...].astype(jnp.float32)
    count = values.shape[0]
    values = values.reshape(count, -1, values.shape[-1])
    sums_ref[0:1, :] = packed(jnp.sum(values, axis=1), members)
    sums_ref[1:2, :] = packed(jnp.sum(values * values, axis=1), members)


def first_sums(frames, members):
    return pl.pallas_call(
        functools.partial(sums_kernel, members),
        out_shape=jax.ShapeDtypeStruct((2, frames.shape[-1]), jnp.float32),
        in_specs=[pl.BlockSpec(memory_space=pltpu.VMEM)],
        out_specs=pl.BlockSpec(memory_space=pltpu.VMEM),
    )(frames)


def masked(flags, edge, rows, wide, side, channels):
    first_row, last_row, first_col, last_col = flags
    row = lax.broadcasted_iota(jnp.int32, (rows, wide, channels), 0)
    col = lax.broadcasted_iota(jnp.int32, (rows, wide, channels), 1)
    far = edge + side
    low_r = jnp.where(first_row == 1, edge, 0)
    high_r = jnp.where(last_row == 1, far, far + edge)
    low_c = jnp.where(first_col == 1, edge, 0)
    high_c = jnp.where(last_col == 1, far, far + edge)
    return (row >= low_r) & (row < high_r) & (col >= low_c) & (col < high_c)


def unfold(act, cols, frame, wide, rows, channels):
    for dy in range(TAPS):
        for dx in range(TAPS):
            at = dy * wide + dx
            tap = (dy * TAPS + dx) * channels
            cols[frame, :rows, tap : tap + channels] = act[frame, at : at + rows].astype(jnp.bfloat16)


def matmul(cols, frame, rows, weights):
    return jnp.dot(cols[frame, :rows], weights, preferred_element_type=jnp.float32)


def context_kernel(side, wide, place_ref, cache_ref, kernel_ref, bias_ref, part_ref, act, cols):
    context = cache_ref.shape[0]
    channels = cache_ref.shape[-1]
    flags = [place_ref[i] for i in range(4)]
    valid = masked(flags, (wide - side) // 2, wide, wide, side, channels)
    rows = (wide - 2) * wide
    for f in range(context):
        values = cache_ref[f].astype(jnp.float32).reshape(wide, wide, channels)
        act[f, : wide * wide] = jnp.where(valid, values, 0.0).reshape(wide * wide, channels)
        act[f, wide * wide :] = jnp.zeros((act.shape[1] - wide * wide, channels), jnp.float32)
        unfold(act, cols, f, wide, rows, channels)
    w0, w1 = kernel_ref[0], kernel_ref[1]
    bias = bias_ref[...].reshape(1, channels)
    pair = matmul(cols, 1, rows, jnp.concatenate([w1, w0], axis=1))
    part_ref[0] = pair[:, :channels] + matmul(cols, 0, rows, w0) + bias
    part_ref[1] = pair[:, channels:] + bias


def context_part(side, wide, place, cache, kernel, bias):
    channels = cache.shape[-1]
    vmem = pl.BlockSpec(memory_space=pltpu.VMEM)
    rows = (wide - 2) * wide
    return pl.pallas_call(
        functools.partial(context_kernel, side, wide),
        out_shape=jax.ShapeDtypeStruct((2, rows, channels), jnp.float32),
        in_specs=[pl.BlockSpec(memory_space=pltpu.SMEM), vmem, vmem, vmem],
        out_specs=vmem,
        scratch_shapes=[
            pltpu.VMEM((cache.shape[0], wide * wide + 8, channels), jnp.float32),
            pltpu.VMEM((cache.shape[0], rows, TAPS * TAPS * channels), jnp.bfloat16),
        ],
        compiler_params=pltpu.CompilerParams(vmem_limit_bytes=VMEM_LIMIT),
        name="context",
    )(place, cache, kernel, bias)


def section_kernel(
    shape, tick, place_ref, x_ref, sums_ref, part_ref, kernel_ref, bias_ref, gain_ref, offset_ref,
    kept_ref, next_ref, result_ref, out_sums_ref, act, held, cols, made,
):
    count, side, wide, _, pixels, members = shape
    rows_in = wide - 2 * tick
    rows_out = rows_in - 2
    channels = x_ref.shape[-1]
    flat_in = rows_in * wide
    flat_out = rows_out * wide
    halo = (wide - side) // 2
    flags = [place_ref[i] for i in range(4)]
    position = place_ref[4]
    mean_row = sums_ref[0:1] / pixels
    square_row = sums_ref[1:2] / pixels
    valid = masked(flags, halo - tick, rows_in, wide, side, channels)
    gain = gain_ref[...].reshape(1, channels)
    offset = offset_ref[...].reshape(1, channels)
    w0, w1, w2 = (kernel_ref[i] for i in range(TAPS))
    both_1 = jnp.concatenate([w1, w0], axis=1)
    both_2 = jnp.concatenate([w2, w1], axis=1)
    bias = bias_ref[...].reshape(1, channels)
    base = tick * (wide + 1)
    edge = halo - tick - 1
    sums, squares = [], []

    def prepare(f):
        mean = unpacked(mean_row, f, members)
        variance = jnp.maximum(unpacked(square_row, f, members) - mean * mean, 0.0)
        scale = gain / jnp.sqrt(variance + EPSILON)
        values = x_ref[f].astype(jnp.float32)
        held[f, :flat_in] = values
        normed = (values - mean) * scale + offset
        half = 0.5 * normed
        active = (half + half * jnp.tanh(half)).reshape(rows_in, wide, channels)
        active = jnp.where(valid, active, 0.0).reshape(flat_in, channels)
        act[f, :flat_in] = active
        unfold(act, cols, f, wide, flat_out, channels)

    def finish(g, value):
        new = value + held[g, wide + 1 : wide + 1 + flat_out]
        new = new.astype(jnp.bfloat16)
        made[g, :flat_out] = new.astype(jnp.float32)
        if next_ref is not None:
            next_ref[g] = new
        total_f = jnp.zeros((side, channels), jnp.float32)
        square_f = jnp.zeros((side, channels), jnp.float32)
        for y in range(side):
            at = (y + edge) * wide + edge
            row = made[g, at : at + side]
            if out_sums_ref is not None:
                total_f = total_f + row
                square_f = square_f + row * row
            row = row.astype(jnp.bfloat16)
            if kept_ref is not None:
                row = jnp.where(position == tick, row, kept_ref[g, y])
            result_ref[g, y] = row
        sums.append(jnp.sum(total_f, axis=0, keepdims=True))
        squares.append(jnp.sum(square_f, axis=0, keepdims=True))

    for f in range(0, count, 2):
        prepare(f)
        pair = matmul(cols, f, flat_out, both_2)
        first, second = pair[:, :channels], pair[:, channels:]
        if f == 0:
            finish(f, first + part_ref[0, base : base + flat_out])
            made[f + 1, :flat_out] = second + part_ref[1, base : base + flat_out]
        else:
            finish(f, first + made[f, :flat_out])
            made[f + 1, :flat_out] = made[f + 1, :flat_out] + second
        if f + 2 < count:
            made[f + 2, :flat_out] = matmul(cols, f, flat_out, w0) + bias
        prepare(f + 1)
        finish(f + 1, matmul(cols, f + 1, flat_out, w2) + made[f + 1, :flat_out])
        if f + 2 < count:
            pair = matmul(cols, f + 1, flat_out, both_1)
            made[f + 2, :flat_out] = made[f + 2, :flat_out] + pair[:, :channels]
            made[f + 3, :flat_out] = pair[:, channels:] + bias
    if out_sums_ref is not None:
        out_sums_ref[0:1, :] = packed(jnp.concatenate(sums, axis=0), members)
        out_sums_ref[1:2, :] = packed(jnp.concatenate(squares, axis=0), members)


def section_step(shape, tick, place, x, sums, part, kernel, bias, gain, offset, kept):
    count, side, wide, sections, _, _ = shape
    channels = x.shape[-1]
    rows_out = wide - 2 * tick - 2
    last = tick == sections - 1
    vmem = pl.BlockSpec(memory_space=pltpu.VMEM)
    inputs = [place, x, sums, part, kernel, bias, gain, offset]
    if kept is not None:
        inputs.append(kept)
    outs = [jax.ShapeDtypeStruct((count, side, side, channels), jnp.bfloat16)]
    if not last:
        outs.insert(0, jax.ShapeDtypeStruct((count, rows_out * wide, channels), jnp.bfloat16))
        outs.append(jax.ShapeDtypeStruct((2, channels), jnp.float32))

    def body(*refs):
        refs = list(refs)
        given = refs[:8]
        del refs[:8]
        kept_ref = refs.pop(0) if kept is not None else None
        next_ref = refs.pop(0) if not last else None
        result_ref = refs.pop(0)
        out_sums_ref = refs.pop(0) if not last else None
        section_kernel(shape, tick, *given, kept_ref, next_ref, result_ref, out_sums_ref, *refs)

    full = wide * wide + 8
    return pl.pallas_call(
        body,
        out_shape=tuple(outs),
        in_specs=[pl.BlockSpec(memory_space=pltpu.SMEM)] + [vmem] * (len(inputs) - 1),
        out_specs=tuple([vmem] * len(outs)),
        scratch_shapes=[
            pltpu.VMEM((count, full, channels), jnp.float32),
            pltpu.VMEM((count, full, channels), jnp.float32),
            pltpu.VMEM((count, rows_out * wide, TAPS * TAPS * channels), jnp.bfloat16),
            pltpu.VMEM((count, rows_out * wide, channels), jnp.float32),
        ],
        compiler_params=pltpu.CompilerParams(vmem_limit_bytes=VMEM_LIMIT),
    )(*inputs)


def local(frames, cache, conv_weight, conv_bias, norm_gain, norm_bias):
    sections = lax.axis_size("section")
    tiles = lax.axis_size("tile")
    across = min(8, tiles // 2)
    down = tiles // across
    position = lax.axis_index("section")
    placed = (lax.axis_index("tile") + across + 2) % tiles
    column, row_at = placed % across, placed // across
    x = frames[:, 0]
    count, side, _, channels = x.shape
    members = channels // GROUPS
    halo = sections
    wide = side + 2 * halo
    pixels = float(side * side * members * tiles)
    shape = (count, side, wide, sections, pixels, members)
    flags = [row_at == 0, row_at == down - 1, column == 0, column == across - 1]
    place = jnp.stack([f.astype(jnp.int32) for f in flags] + [position.astype(jnp.int32)])
    kernel = conv_weight[0].reshape(TAPS, TAPS * TAPS * channels, channels)

    old = cache[0, :, 0]
    context = old.shape[0]
    sums = first_sums(x, members)
    seq = jnp.concatenate([old, x], axis=0)
    left = shifted(seq[:, :, side - halo :], 1)
    right = shifted(seq[:, :, :halo], -1)
    middle = jnp.concatenate([left, seq, right], axis=2)
    above = shifted(middle[:, side - halo :], across)
    below = shifted(middle[:, :halo], -across)
    sums = of_everyone(sums)
    held_cache, x = (
        jnp.concatenate([above[c], middle[c], below[c]], axis=1).reshape(-1, wide * wide, channels)
        for c in (slice(0, context), slice(context, None))
    )
    part = context_part(side, wide, place, held_cache, kernel, conv_bias)

    result = None
    for tick in range(sections):
        made = section_step(
            shape, tick, place, x, sums, part, kernel, conv_bias, norm_gain, norm_bias, result
        )
        if tick + 1 == sections:
            (result,) = made
            break
        x, result, sums = made
        hop = [(tick, tick + 1)]
        sums = lax.ppermute(sums, "section", hop)
        x = lax.ppermute(x, "section", hop)
        sums = of_everyone(sums)
    return result[None, :, None]


def solution(mesh):
    placed = (
        P("parts", "tile", None, None, None),
        P("section", "parts", "tile", None, None, None),
        P("section", None, None, None, None, None),
        P("section", None),
        P("section", None),
        P("section", None),
    )
    return jax.shard_map(
        local,
        mesh=mesh,
        in_specs=placed,
        out_specs=P("section", "parts", "tile", None, None, None),
        check_vma=False,
    )
```

```python
import functools

import jax
import jax.numpy as jnp
from jax import lax
from jax.experimental import pallas as pl
from jax.experimental.pallas import tpu as pltpu
from jax.sharding import PartitionSpec as P


GROUPS = 32
EPSILON = 1e-06
TAPS = 3
VMEM_LIMIT = 20 * 1024 * 1024


def shifted(array, by):
    peers = lax.axis_size("tile")
    return lax.ppermute(array, "tile", [(i, (i + by) % peers) for i in range(peers)])


def both_cores(sums):
    pairs = [[i, i + 1] for i in range(0, lax.axis_size("tile"), 2)]
    return jnp.sum(lax.all_gather(sums, "tile", axis_index_groups=pairs), axis=0)


def to_next(sums, section):
    tiles = lax.axis_size("tile")
    axes = ("section", "tile")
    here, there = section * tiles, (section + 1) * tiles
    same = lax.ppermute(sums, axes, [(here + t, there + t) for t in range(tiles)])
    other = lax.ppermute(sums, axes, [(here + t, there + (t ^ 1)) for t in range(tiles)])
    return same + other


def of_everyone(sums):
    chips = lax.axis_size("tile") // 2
    groups = [[core + 2 * i for i in range(chips)] for core in range(2)]
    copies = jnp.broadcast_to(sums.reshape(1, 1, sums.size), (chips, 1, sums.size))
    all_sums = lax.all_to_all(copies, "tile", 0, 0, tiled=True, axis_index_groups=groups)
    return jnp.sum(all_sums, axis=0).reshape(sums.shape)


def swapped(array, across, first):
    tiles = lax.axis_size("tile")
    pairs = []
    for t in range(tiles):
        placed = (t + across + 2) % tiles
        down = ((placed // across) % 2 == 0) == first
        pairs.append((t, (t + (across if down else -across)) % tiles))
    return lax.ppermute(array, "tile", pairs)


def over_lanes(value, members):
    lanes = value.shape[-1]
    lane = lax.broadcasted_iota(jnp.int32, value.shape, value.ndim - 1)
    step = 1
    while step < members:
        up = pltpu.roll(value, lanes - step, value.ndim - 1)
        down = pltpu.roll(value, step, value.ndim - 1)
        value = value + jnp.where((lane // step) % 2 == 0, up, down)
        step *= 2
    return value


def packed(totals, members):
    totals = over_lanes(totals, members)
    lane = lax.broadcasted_iota(jnp.int32, (1, totals.shape[-1]), 1)
    row = jnp.zeros((1, totals.shape[-1]), jnp.float32)
    for frame in range(totals.shape[0]):
        row = row + jnp.where(lane % members == frame, totals[frame : frame + 1], 0.0)
    return row


def unpacked(row, frame, members):
    lane = lax.broadcasted_iota(jnp.int32, row.shape, 1)
    return over_lanes(jnp.where(lane % members == frame, row, 0.0), members)


def sums_kernel(members, x_ref, sums_ref):
    values = x_ref[...].astype(jnp.float32)
    count = values.shape[0]
    values = values.reshape(count, -1, values.shape[-1])
    sums_ref[0:1, :] = packed(jnp.sum(values, axis=1), members)
    sums_ref[1:2, :] = packed(jnp.sum(values * values, axis=1), members)


def first_sums(frames, members):
    return pl.pallas_call(
        functools.partial(sums_kernel, members),
        out_shape=jax.ShapeDtypeStruct((2, frames.shape[-1]), jnp.float32),
        in_specs=[pl.BlockSpec(memory_space=pltpu.VMEM)],
        out_specs=pl.BlockSpec(memory_space=pltpu.VMEM),
        compiler_params=pltpu.CompilerParams(vmem_limit_bytes=VMEM_LIMIT),
        name="first_sums",
    )(frames)


def masked(flags, edge, rows, wide, side, channels):
    first_row, last_row, first_col, last_col = flags
    row = lax.broadcasted_iota(jnp.int32, (rows, wide, channels), 0)
    col = lax.broadcasted_iota(jnp.int32, (rows, wide, channels), 1)
    far = edge + side
    low_r = jnp.where(first_row == 1, edge, 0)
    high_r = jnp.where(last_row == 1, far, far + edge)
    low_c = jnp.where(first_col == 1, edge, 0)
    high_c = jnp.where(last_col == 1, far, far + edge)
    return (row >= low_r) & (row < high_r) & (col >= low_c) & (col < high_c)


def unfold(act, cols, frame, wide, rows, channels):
    for dy in range(TAPS):
        for dx in range(TAPS):
            at = dy * wide + dx
            tap = (dy * TAPS + dx) * channels
            cols[frame, :rows, tap : tap + channels] = act[frame, at : at + rows].astype(jnp.bfloat16)


def matmul(cols, frame, rows, weights):
    return jnp.dot(cols[frame, :rows], weights, preferred_element_type=jnp.float32)


def context_kernel(side, wide, place_ref, cache_ref, kernel_ref, bias_ref, part_ref, act, cols):
    context = cache_ref.shape[0]
    channels = cache_ref.shape[-1]
    flags = [place_ref[i] for i in range(4)]
    valid = masked(flags, (wide - side) // 2, wide, wide, side, channels)
    rows = (wide - 2) * wide
    for f in range(context):
        values = cache_ref[f].astype(jnp.float32).reshape(wide, wide, channels)
        act[f, : wide * wide] = jnp.where(valid, values, 0.0).reshape(wide * wide, channels)
        act[f, wide * wide :] = jnp.zeros((act.shape[1] - wide * wide, channels), jnp.float32)
        unfold(act, cols, f, wide, rows, channels)
    w0, w1 = kernel_ref[0], kernel_ref[1]
    bias = bias_ref[...].reshape(1, channels)
    pair = matmul(cols, 1, rows, jnp.concatenate([w1, w0], axis=1))
    part_ref[0] = pair[:, :channels] + matmul(cols, 0, rows, w0) + bias
    part_ref[1] = pair[:, channels:] + bias


def context_part(side, wide, place, cache, kernel, bias):
    channels = cache.shape[-1]
    vmem = pl.BlockSpec(memory_space=pltpu.VMEM)
    rows = (wide - 2) * wide
    return pl.pallas_call(
        functools.partial(context_kernel, side, wide),
        out_shape=jax.ShapeDtypeStruct((2, rows, channels), jnp.float32),
        in_specs=[pl.BlockSpec(memory_space=pltpu.SMEM), vmem, vmem, vmem],
        out_specs=vmem,
        scratch_shapes=[
            pltpu.VMEM((cache.shape[0], wide * wide + 8, channels), jnp.float32),
            pltpu.VMEM((cache.shape[0], rows, TAPS * TAPS * channels), jnp.bfloat16),
        ],
        compiler_params=pltpu.CompilerParams(vmem_limit_bytes=VMEM_LIMIT),
        name="context",
    )(place, cache, kernel, bias)


def section_kernel(
    shape, tick, place_ref, x_ref, sums_ref, part_ref, kernel_ref, bias_ref, gain_ref, offset_ref,
    kept_ref, next_ref, result_ref, out_sums_ref, act, held, cols, made,
):
    count, side, wide, _, pixels, members = shape
    rows_in = wide - 2 * tick
    rows_out = rows_in - 2
    channels = x_ref.shape[-1]
    flat_in = rows_in * wide
    flat_out = rows_out * wide
    halo = (wide - side) // 2
    flags = [place_ref[i] for i in range(4)]
    position = place_ref[4]
    mean_row = sums_ref[0:1] / pixels
    square_row = sums_ref[1:2] / pixels
    valid = masked(flags, halo - tick, rows_in, wide, side, channels)
    gain = gain_ref[...].reshape(1, channels)
    offset = offset_ref[...].reshape(1, channels)
    w0, w1, w2 = (kernel_ref[i] for i in range(TAPS))
    both_1 = jnp.concatenate([w1, w0], axis=1)
    both_2 = jnp.concatenate([w2, w1], axis=1)
    bias = bias_ref[...].reshape(1, channels)
    base = tick * (wide + 1)
    edge = halo - tick - 1
    sums, squares = [], []

    def prepare(f):
        mean = unpacked(mean_row, f, members)
        variance = jnp.maximum(unpacked(square_row, f, members) - mean * mean, 0.0)
        scale = gain / jnp.sqrt(variance + EPSILON)
        values = x_ref[f].astype(jnp.float32)
        held[f, :flat_in] = values
        normed = (values - mean) * scale + offset
        half = 0.5 * normed
        active = (half + half * jnp.tanh(half)).reshape(rows_in, wide, channels)
        active = jnp.where(valid, active, 0.0).reshape(flat_in, channels)
        act[f, :flat_in] = active
        unfold(act, cols, f, wide, flat_out, channels)

    def finish(g, value):
        new = value + held[g, wide + 1 : wide + 1 + flat_out]
        new = new.astype(jnp.bfloat16)
        made[g, :flat_out] = new.astype(jnp.float32)
        if next_ref is not None:
            next_ref[g] = new
        total_f = jnp.zeros((side, channels), jnp.float32)
        square_f = jnp.zeros((side, channels), jnp.float32)
        for y in range(side):
            at = (y + edge) * wide + edge
            row = made[g, at : at + side]
            if out_sums_ref is not None:
                total_f = total_f + row
                square_f = square_f + row * row
            row = row.astype(jnp.bfloat16)
            if kept_ref is not None:
                row = jnp.where(position == tick, row, kept_ref[g, y])
            result_ref[g, y] = row
        sums.append(jnp.sum(total_f, axis=0, keepdims=True))
        squares.append(jnp.sum(square_f, axis=0, keepdims=True))

    for f in range(0, count, 2):
        prepare(f)
        pair = matmul(cols, f, flat_out, both_2)
        first, second = pair[:, :channels], pair[:, channels:]
        if f == 0:
            finish(f, first + part_ref[0, base : base + flat_out])
            made[f + 1, :flat_out] = second + part_ref[1, base : base + flat_out]
        else:
            finish(f, first + made[f, :flat_out])
            made[f + 1, :flat_out] = made[f + 1, :flat_out] + second
        if f + 2 < count:
            made[f + 2, :flat_out] = matmul(cols, f, flat_out, w0) + bias
        prepare(f + 1)
        finish(f + 1, matmul(cols, f + 1, flat_out, w2) + made[f + 1, :flat_out])
        if f + 2 < count:
            pair = matmul(cols, f + 1, flat_out, both_1)
            made[f + 2, :flat_out] = made[f + 2, :flat_out] + pair[:, :channels]
            made[f + 3, :flat_out] = pair[:, channels:] + bias
    if out_sums_ref is not None:
        out_sums_ref[0:1, :] = packed(jnp.concatenate(sums, axis=0), members)
        out_sums_ref[1:2, :] = packed(jnp.concatenate(squares, axis=0), members)


def section_step(shape, tick, place, x, sums, part, kernel, bias, gain, offset, kept):
    count, side, wide, sections, _, _ = shape
    channels = x.shape[-1]
    rows_out = wide - 2 * tick - 2
    last = tick == sections - 1
    vmem = pl.BlockSpec(memory_space=pltpu.VMEM)
    inputs = [place, x, sums, part, kernel, bias, gain, offset]
    if kept is not None:
        inputs.append(kept)
    outs = [jax.ShapeDtypeStruct((count, side, side, channels), jnp.bfloat16)]
    if not last:
        outs.insert(0, jax.ShapeDtypeStruct((count, rows_out * wide, channels), jnp.bfloat16))
        outs.append(jax.ShapeDtypeStruct((2, channels), jnp.float32))

    def body(*refs):
        refs = list(refs)
        given = refs[:8]
        del refs[:8]
        kept_ref = refs.pop(0) if kept is not None else None
        next_ref = refs.pop(0) if not last else None
        result_ref = refs.pop(0)
        out_sums_ref = refs.pop(0) if not last else None
        section_kernel(shape, tick, *given, kept_ref, next_ref, result_ref, out_sums_ref, *refs)

    full = wide * wide + 8
    return pl.pallas_call(
        body,
        out_shape=tuple(outs),
        in_specs=[pl.BlockSpec(memory_space=pltpu.SMEM)] + [vmem] * (len(inputs) - 1),
        out_specs=tuple([vmem] * len(outs)),
        scratch_shapes=[
            pltpu.VMEM((count, full, channels), jnp.float32),
            pltpu.VMEM((count, full, channels), jnp.float32),
            pltpu.VMEM((count, rows_out * wide, TAPS * TAPS * channels), jnp.bfloat16),
            pltpu.VMEM((count, rows_out * wide, channels), jnp.float32),
        ],
        compiler_params=pltpu.CompilerParams(vmem_limit_bytes=VMEM_LIMIT),
    )(*inputs)


def local(frames, cache, conv_weight, conv_bias, norm_gain, norm_bias):
    sections = lax.axis_size("section")
    tiles = lax.axis_size("tile")
    across = min(8, tiles // 2)
    down = tiles // across
    position = lax.axis_index("section")
    placed = (lax.axis_index("tile") + across + 2) % tiles
    column, row_at = placed % across, placed // across
    x = frames[:, 0]
    count, side, _, channels = x.shape
    members = channels // GROUPS
    halo = sections
    wide = side + 2 * halo
    pixels = float(side * side * members * tiles)
    shape = (count, side, wide, sections, pixels, members)
    flags = [row_at == 0, row_at == down - 1, column == 0, column == across - 1]
    place = jnp.stack([f.astype(jnp.int32) for f in flags] + [position.astype(jnp.int32)])
    kernel = conv_weight[0].reshape(TAPS, TAPS * TAPS * channels, channels)

    old = cache[0, :, 0]
    context = old.shape[0]
    sums = first_sums(x, members)
    seq = jnp.concatenate([old, x], axis=0)
    left = shifted(seq[:, :, side - halo :], 1)
    right = shifted(seq[:, :, :halo], -1)
    middle = jnp.concatenate([left, seq, right], axis=2)
    even = row_at % 2 == 0
    top, bottom = middle[:, :halo], middle[:, side - halo :]
    one = swapped(jnp.where(even, bottom, top), across, True)
    two = swapped(jnp.where(even, top, bottom), across, False)
    above = jnp.where(even, two, one)
    below = jnp.where(even, one, two)
    sums = both_cores(sums)
    sums = of_everyone(sums)
    held_cache, x = (
        jnp.concatenate([above[c], middle[c], below[c]], axis=1).reshape(-1, wide * wide, channels)
        for c in (slice(0, context), slice(context, None))
    )
    part = context_part(side, wide, place, held_cache, kernel, conv_bias)

    result = None
    for tick in range(sections):
        made = section_step(
            shape, tick, place, x, sums, part, kernel, conv_bias, norm_gain, norm_bias, result
        )
        if tick + 1 == sections:
            (result,) = made
            break
        x, result, sums = made
        hop = [(tick, tick + 1)]
        sums = to_next(sums, tick)
        x = lax.ppermute(x, "section", hop)
        sums = of_everyone(sums)
    return result[None, :, None]


def solution(mesh):
    placed = (
        P("parts", "tile", None, None, None),
        P("section", "parts", "tile", None, None, None),
        P("section", None, None, None, None, None),
        P("section", None),
        P("section", None),
        P("section", None),
    )
    return jax.shard_map(
        local,
        mesh=mesh,
        in_specs=placed,
        out_specs=P("section", "parts", "tile", None, None, None),
        check_vma=False,
    )
```

```python
import functools

import jax
import jax.numpy as jnp
from jax import lax
from jax.experimental import pallas as pl
from jax.experimental.pallas import tpu as pltpu
from jax.sharding import PartitionSpec as P


GROUPS = 32
EPSILON = 1e-06
TAPS = 3
VMEM_LIMIT = 20 * 1024 * 1024


def shifted(array, by):
    peers = lax.axis_size("tile")
    return lax.ppermute(array, "tile", [(i, (i + by) % peers) for i in range(peers)])


def both_cores(sums):
    pairs = [[i, i + 1] for i in range(0, lax.axis_size("tile"), 2)]
    return jnp.sum(lax.all_gather(sums, "tile", axis_index_groups=pairs), axis=0)


def to_next(sums, section):
    tiles = lax.axis_size("tile")
    axes = ("section", "tile")
    here, there = section * tiles, (section + 1) * tiles
    same = lax.ppermute(sums, axes, [(here + t, there + t) for t in range(tiles)])
    other = lax.ppermute(sums, axes, [(here + t, there + (t ^ 1)) for t in range(tiles)])
    return same + other


def of_everyone(sums):
    chips = lax.axis_size("tile") // 2
    ends = [i // 2 if i % 2 == 0 else chips - 1 - i // 2 for i in range(chips)]
    groups = [[core + 2 * i for i in ends] for core in range(2)]
    copies = jnp.broadcast_to(sums.reshape(1, 1, sums.size), (chips, 1, sums.size))
    all_sums = lax.all_to_all(copies, "tile", 0, 0, tiled=True, axis_index_groups=groups)
    return jnp.sum(all_sums, axis=0).reshape(sums.shape)


def over_lanes(value, members):
    lanes = value.shape[-1]
    lane = lax.broadcasted_iota(jnp.int32, value.shape, value.ndim - 1)
    step = 1
    while step < members:
        up = pltpu.roll(value, lanes - step, value.ndim - 1)
        down = pltpu.roll(value, step, value.ndim - 1)
        value = value + jnp.where((lane // step) % 2 == 0, up, down)
        step *= 2
    return value


def packed(totals, members):
    totals = over_lanes(totals, members)
    lane = lax.broadcasted_iota(jnp.int32, (1, totals.shape[-1]), 1)
    row = jnp.zeros((1, totals.shape[-1]), jnp.float32)
    for frame in range(totals.shape[0]):
        row = row + jnp.where(lane % members == frame, totals[frame : frame + 1], 0.0)
    return row


def unpacked(row, frame, members):
    lane = lax.broadcasted_iota(jnp.int32, row.shape, 1)
    return over_lanes(jnp.where(lane % members == frame, row, 0.0), members)


def sums_kernel(count, members, x_ref, sums_ref):
    values = x_ref[x_ref.shape[0] - count :].astype(jnp.float32)
    values = values.reshape(count, -1, values.shape[-1])
    sums_ref[0:1, :] = packed(jnp.sum(values, axis=1), members)
    sums_ref[1:2, :] = packed(jnp.sum(values * values, axis=1), members)


def first_sums(frames, count, members):
    return pl.pallas_call(
        functools.partial(sums_kernel, count, members),
        out_shape=jax.ShapeDtypeStruct((2, frames.shape[-1]), jnp.float32),
        in_specs=[pl.BlockSpec(memory_space=pltpu.VMEM)],
        out_specs=pl.BlockSpec(memory_space=pltpu.VMEM),
        compiler_params=pltpu.CompilerParams(vmem_limit_bytes=VMEM_LIMIT),
        name="first_sums",
    )(frames)


def masked(flags, edge, rows, wide, side, channels):
    first_row, last_row, first_col, last_col = flags
    row = lax.broadcasted_iota(jnp.int32, (rows, wide, channels), 0)
    col = lax.broadcasted_iota(jnp.int32, (rows, wide, channels), 1)
    far = edge + side
    low_r = jnp.where(first_row == 1, edge, 0)
    high_r = jnp.where(last_row == 1, far, far + edge)
    low_c = jnp.where(first_col == 1, edge, 0)
    high_c = jnp.where(last_col == 1, far, far + edge)
    return (row >= low_r) & (row < high_r) & (col >= low_c) & (col < high_c)


def unfold(act, cols, frame, wide, rows, channels):
    for dy in range(TAPS):
        for dx in range(TAPS):
            at = dy * wide + dx
            tap = (dy * TAPS + dx) * channels
            cols[frame, :rows, tap : tap + channels] = act[frame, at : at + rows].astype(jnp.bfloat16)


def matmul(cols, frame, rows, weights):
    return jnp.dot(cols[frame, :rows], weights, preferred_element_type=jnp.float32)


def context_kernel(side, wide, place_ref, cache_ref, kernel_ref, bias_ref, part_ref, act, cols):
    context = cache_ref.shape[0]
    channels = cache_ref.shape[-1]
    flags = [place_ref[i] for i in range(4)]
    valid = masked(flags, (wide - side) // 2, wide, wide, side, channels)
    rows = (wide - 2) * wide
    for f in range(context):
        values = cache_ref[f].astype(jnp.float32).reshape(wide, wide, channels)
        act[f, : wide * wide] = jnp.where(valid, values, 0.0).reshape(wide * wide, channels)
        act[f, wide * wide :] = jnp.zeros((act.shape[1] - wide * wide, channels), jnp.float32)
        unfold(act, cols, f, wide, rows, channels)
    w0, w1 = kernel_ref[0], kernel_ref[1]
    bias = bias_ref[...].reshape(1, channels)
    pair = matmul(cols, 1, rows, jnp.concatenate([w1, w0], axis=1))
    part_ref[0] = pair[:, :channels] + matmul(cols, 0, rows, w0) + bias
    part_ref[1] = pair[:, channels:] + bias


def context_part(side, wide, place, cache, kernel, bias):
    channels = cache.shape[-1]
    vmem = pl.BlockSpec(memory_space=pltpu.VMEM)
    rows = (wide - 2) * wide
    return pl.pallas_call(
        functools.partial(context_kernel, side, wide),
        out_shape=jax.ShapeDtypeStruct((2, rows, channels), jnp.float32),
        in_specs=[pl.BlockSpec(memory_space=pltpu.SMEM), vmem, vmem, vmem],
        out_specs=vmem,
        scratch_shapes=[
            pltpu.VMEM((cache.shape[0], wide * wide + 8, channels), jnp.float32),
            pltpu.VMEM((cache.shape[0], rows, TAPS * TAPS * channels), jnp.bfloat16),
        ],
        compiler_params=pltpu.CompilerParams(vmem_limit_bytes=VMEM_LIMIT),
        name="context",
    )(place, cache, kernel, bias)


def section_kernel(
    shape, tick, place_ref, x_ref, sums_ref, part_ref, kernel_ref, bias_ref, gain_ref, offset_ref,
    kept_ref, next_ref, result_ref, out_sums_ref, act, held, cols, made,
):
    count, side, wide, _, pixels, members = shape
    rows_in = wide - 2 * tick
    rows_out = rows_in - 2
    channels = x_ref.shape[-1]
    flat_in = rows_in * wide
    flat_out = rows_out * wide
    halo = (wide - side) // 2
    flags = [place_ref[i] for i in range(4)]
    position = place_ref[4]
    mean_row = sums_ref[0:1] / pixels
    square_row = sums_ref[1:2] / pixels
    valid = masked(flags, halo - tick, rows_in, wide, side, channels)
    gain = gain_ref[...].reshape(1, channels)
    offset = offset_ref[...].reshape(1, channels)
    w0, w1, w2 = (kernel_ref[i] for i in range(TAPS))
    both_1 = jnp.concatenate([w1, w0], axis=1)
    both_2 = jnp.concatenate([w2, w1], axis=1)
    bias = bias_ref[...].reshape(1, channels)
    base = tick * (wide + 1)
    edge = halo - tick - 1
    sums, squares = [], []

    def prepare(f):
        mean = unpacked(mean_row, f, members)
        variance = jnp.maximum(unpacked(square_row, f, members) - mean * mean, 0.0)
        scale = gain / jnp.sqrt(variance + EPSILON)
        values = x_ref[f].astype(jnp.float32)
        held[f, :flat_in] = values
        normed = (values - mean) * scale + offset
        half = 0.5 * normed
        active = (half + half * jnp.tanh(half)).reshape(rows_in, wide, channels)
        active = jnp.where(valid, active, 0.0).reshape(flat_in, channels)
        act[f, :flat_in] = active
        unfold(act, cols, f, wide, flat_out, channels)

    def finish(g, value):
        new = value + held[g, wide + 1 : wide + 1 + flat_out]
        new = new.astype(jnp.bfloat16)
        made[g, :flat_out] = new.astype(jnp.float32)
        if next_ref is not None:
            next_ref[g] = new
        total_f = jnp.zeros((side, channels), jnp.float32)
        square_f = jnp.zeros((side, channels), jnp.float32)
        for y in range(side):
            at = (y + edge) * wide + edge
            row = made[g, at : at + side]
            if out_sums_ref is not None:
                total_f = total_f + row
                square_f = square_f + row * row
            row = row.astype(jnp.bfloat16)
            if kept_ref is not None:
                row = jnp.where(position == tick, row, kept_ref[g, y])
            result_ref[g, y] = row
        sums.append(jnp.sum(total_f, axis=0, keepdims=True))
        squares.append(jnp.sum(square_f, axis=0, keepdims=True))

    for f in range(0, count, 2):
        prepare(f)
        pair = matmul(cols, f, flat_out, both_2)
        first, second = pair[:, :channels], pair[:, channels:]
        if f == 0:
            finish(f, first + part_ref[0, base : base + flat_out])
            made[f + 1, :flat_out] = second + part_ref[1, base : base + flat_out]
        else:
            finish(f, first + made[f, :flat_out])
            made[f + 1, :flat_out] = made[f + 1, :flat_out] + second
        if f + 2 < count:
            made[f + 2, :flat_out] = matmul(cols, f, flat_out, w0) + bias
        prepare(f + 1)
        finish(f + 1, matmul(cols, f + 1, flat_out, w2) + made[f + 1, :flat_out])
        if f + 2 < count:
            pair = matmul(cols, f + 1, flat_out, both_1)
            made[f + 2, :flat_out] = made[f + 2, :flat_out] + pair[:, :channels]
            made[f + 3, :flat_out] = pair[:, channels:] + bias
    if out_sums_ref is not None:
        out_sums_ref[0:1, :] = packed(jnp.concatenate(sums, axis=0), members)
        out_sums_ref[1:2, :] = packed(jnp.concatenate(squares, axis=0), members)


def section_step(shape, tick, place, x, sums, part, kernel, bias, gain, offset, kept):
    count, side, wide, sections, _, _ = shape
    channels = x.shape[-1]
    rows_out = wide - 2 * tick - 2
    last = tick == sections - 1
    vmem = pl.BlockSpec(memory_space=pltpu.VMEM)
    inputs = [place, x, sums, part, kernel, bias, gain, offset]
    if kept is not None:
        inputs.append(kept)
    outs = [jax.ShapeDtypeStruct((count, side, side, channels), jnp.bfloat16)]
    if not last:
        outs.insert(0, jax.ShapeDtypeStruct((count, rows_out * wide, channels), jnp.bfloat16))
        outs.append(jax.ShapeDtypeStruct((2, channels), jnp.float32))

    def body(*refs):
        refs = list(refs)
        given = refs[:8]
        del refs[:8]
        kept_ref = refs.pop(0) if kept is not None else None
        next_ref = refs.pop(0) if not last else None
        result_ref = refs.pop(0)
        out_sums_ref = refs.pop(0) if not last else None
        section_kernel(shape, tick, *given, kept_ref, next_ref, result_ref, out_sums_ref, *refs)

    full = wide * wide + 8
    return pl.pallas_call(
        body,
        out_shape=tuple(outs),
        in_specs=[pl.BlockSpec(memory_space=pltpu.SMEM)] + [vmem] * (len(inputs) - 1),
        out_specs=tuple([vmem] * len(outs)),
        scratch_shapes=[
            pltpu.VMEM((count, full, channels), jnp.float32),
            pltpu.VMEM((count, full, channels), jnp.float32),
            pltpu.VMEM((count, rows_out * wide, TAPS * TAPS * channels), jnp.bfloat16),
            pltpu.VMEM((count, rows_out * wide, channels), jnp.float32),
        ],
        compiler_params=pltpu.CompilerParams(vmem_limit_bytes=VMEM_LIMIT),
    )(*inputs)


def local(frames, cache, conv_weight, conv_bias, norm_gain, norm_bias):
    sections = lax.axis_size("section")
    tiles = lax.axis_size("tile")
    across = min(8, tiles // 2)
    down = tiles // across
    position = lax.axis_index("section")
    placed = (lax.axis_index("tile") + across + 2) % tiles
    column, row_at = placed % across, placed // across
    x = frames[:, 0]
    count, side, _, channels = x.shape
    members = channels // GROUPS
    halo = sections
    wide = side + 2 * halo
    pixels = float(side * side * members * tiles)
    shape = (count, side, wide, sections, pixels, members)
    flags = [row_at == 0, row_at == down - 1, column == 0, column == across - 1]
    place = jnp.stack([f.astype(jnp.int32) for f in flags] + [position.astype(jnp.int32)])
    kernel = conv_weight[0].reshape(TAPS, TAPS * TAPS * channels, channels)

    old = cache[0, :, 0]
    context = old.shape[0]
    seq = lax.optimization_barrier(jnp.concatenate([old, x], axis=0))
    left = shifted(seq[:, :, side - halo :], 1)
    right = shifted(seq[:, :, :halo], -1)
    sums = both_cores(first_sums(seq, count, members))
    left, right, sums = lax.optimization_barrier((left, right, sums))
    middle = jnp.concatenate([left, seq, right], axis=2)
    above = shifted(middle[:, side - halo :], across)
    below = shifted(middle[:, :halo], -across)
    sums = of_everyone(sums)
    held_cache, x = (
        jnp.concatenate([above[c], middle[c], below[c]], axis=1).reshape(-1, wide * wide, channels)
        for c in (slice(0, context), slice(context, None))
    )
    part = context_part(side, wide, place, held_cache, kernel, conv_bias)

    result = None
    for tick in range(sections):
        made = section_step(
            shape, tick, place, x, sums, part, kernel, conv_bias, norm_gain, norm_bias, result
        )
        if tick + 1 == sections:
            (result,) = made
            break
        x, result, sums = made
        hop = [(tick, tick + 1)]
        sums = to_next(sums, tick)
        x = lax.ppermute(x, "section", hop)
        sums = of_everyone(sums)
    return result[None, :, None]


def solution(mesh):
    placed = (
        P("parts", "tile", None, None, None),
        P("section", "parts", "tile", None, None, None),
        P("section", None, None, None, None, None),
        P("section", None),
        P("section", None),
        P("section", None),
    )
    return jax.shard_map(
        local,
        mesh=mesh,
        in_specs=placed,
        out_specs=P("section", "parts", "tile", None, None, None),
        check_vma=False,
    )
```

```python
import functools

import jax
import jax.numpy as jnp
from jax import lax
from jax.experimental import pallas as pl
from jax.experimental.pallas import tpu as pltpu
from jax.sharding import PartitionSpec as P


GROUPS = 32
EPSILON = 1e-06
TAPS = 3
VMEM_LIMIT = 20 * 1024 * 1024


def shifted(array, by):
    peers = lax.axis_size("tile")
    return lax.ppermute(array, "tile", [(i, (i + by) % peers) for i in range(peers)])


def both_cores(sums):
    pairs = [[i, i + 1] for i in range(0, lax.axis_size("tile"), 2)]
    return jnp.sum(lax.all_gather(sums, "tile", axis_index_groups=pairs), axis=0)


def to_next(sums, section):
    tiles = lax.axis_size("tile")
    axes = ("section", "tile")
    here, there = section * tiles, (section + 1) * tiles
    same = lax.ppermute(sums, axes, [(here + t, there + t) for t in range(tiles)])
    other = lax.ppermute(sums, axes, [(here + t, there + (t ^ 1)) for t in range(tiles)])
    return same + other


def of_everyone(sums):
    chips = lax.axis_size("tile") // 2
    ends = [i // 2 if i % 2 == 0 else chips - 1 - i // 2 for i in range(chips)]
    groups = [[core + 2 * i for i in ends] for core in range(2)]
    copies = jnp.broadcast_to(sums.reshape(1, 1, sums.size), (chips, 1, sums.size))
    all_sums = lax.all_to_all(copies, "tile", 0, 0, tiled=True, axis_index_groups=groups)
    return jnp.sum(all_sums, axis=0).reshape(sums.shape)


def over_lanes(value, members):
    lanes = value.shape[-1]
    lane = lax.broadcasted_iota(jnp.int32, value.shape, value.ndim - 1)
    step = 1
    while step < members:
        up = pltpu.roll(value, lanes - step, value.ndim - 1)
        down = pltpu.roll(value, step, value.ndim - 1)
        value = value + jnp.where((lane // step) % 2 == 0, up, down)
        step *= 2
    return value


def packed(totals, members):
    totals = over_lanes(totals, members)
    lane = lax.broadcasted_iota(jnp.int32, (1, totals.shape[-1]), 1)
    row = jnp.zeros((1, totals.shape[-1]), jnp.float32)
    for frame in range(totals.shape[0]):
        row = row + jnp.where(lane % members == frame, totals[frame : frame + 1], 0.0)
    return row


def unpacked(row, frame, members):
    lane = lax.broadcasted_iota(jnp.int32, row.shape, 1)
    return over_lanes(jnp.where(lane % members == frame, row, 0.0), members)


def sums_kernel(count, members, x_ref, sums_ref):
    values = x_ref[x_ref.shape[0] - count :].astype(jnp.float32)
    values = values.reshape(count, -1, values.shape[-1])
    sums_ref[0:1, :] = packed(jnp.sum(values, axis=1), members)
    sums_ref[1:2, :] = packed(jnp.sum(values * values, axis=1), members)


def first_sums(frames, count, members):
    return pl.pallas_call(
        functools.partial(sums_kernel, count, members),
        out_shape=jax.ShapeDtypeStruct((2, frames.shape[-1]), jnp.float32),
        in_specs=[pl.BlockSpec(memory_space=pltpu.VMEM)],
        out_specs=pl.BlockSpec(memory_space=pltpu.VMEM),
        compiler_params=pltpu.CompilerParams(vmem_limit_bytes=VMEM_LIMIT),
        name="first_sums",
    )(frames)


def masked(flags, edge, rows, wide, side, channels):
    first_row, last_row, first_col, last_col = flags
    row = lax.broadcasted_iota(jnp.int32, (rows, wide, channels), 0)
    col = lax.broadcasted_iota(jnp.int32, (rows, wide, channels), 1)
    far = edge + side
    low_r = jnp.where(first_row == 1, edge, 0)
    high_r = jnp.where(last_row == 1, far, far + edge)
    low_c = jnp.where(first_col == 1, edge, 0)
    high_c = jnp.where(last_col == 1, far, far + edge)
    return (row >= low_r) & (row < high_r) & (col >= low_c) & (col < high_c)


def unfold(act, cols, frame, wide, rows, channels):
    for dy in range(TAPS):
        for dx in range(TAPS):
            at = dy * wide + dx
            tap = (dy * TAPS + dx) * channels
            cols[frame, :rows, tap : tap + channels] = act[frame, at : at + rows].astype(jnp.bfloat16)


def matmul(cols, frame, rows, weights):
    return jnp.dot(cols[frame, :rows], weights, preferred_element_type=jnp.float32)


def context_kernel(side, wide, place_ref, cache_ref, kernel_ref, bias_ref, part_ref, act, cols):
    context = cache_ref.shape[0]
    channels = cache_ref.shape[-1]
    flags = [place_ref[i] for i in range(4)]
    valid = masked(flags, (wide - side) // 2, wide, wide, side, channels)
    rows = (wide - 2) * wide
    for f in range(context):
        values = cache_ref[f].astype(jnp.float32).reshape(wide, wide, channels)
        act[f, : wide * wide] = jnp.where(valid, values, 0.0).reshape(wide * wide, channels)
        act[f, wide * wide :] = jnp.zeros((act.shape[1] - wide * wide, channels), jnp.float32)
        unfold(act, cols, f, wide, rows, channels)
    w0, w1 = kernel_ref[0], kernel_ref[1]
    bias = bias_ref[...].reshape(1, channels)
    pair = matmul(cols, 1, rows, jnp.concatenate([w1, w0], axis=1))
    part_ref[0] = pair[:, :channels] + matmul(cols, 0, rows, w0) + bias
    part_ref[1] = pair[:, channels:] + bias


def context_part(side, wide, place, cache, kernel, bias):
    channels = cache.shape[-1]
    vmem = pl.BlockSpec(memory_space=pltpu.VMEM)
    rows = (wide - 2) * wide
    return pl.pallas_call(
        functools.partial(context_kernel, side, wide),
        out_shape=jax.ShapeDtypeStruct((2, rows, channels), jnp.float32),
        in_specs=[pl.BlockSpec(memory_space=pltpu.SMEM), vmem, vmem, vmem],
        out_specs=vmem,
        scratch_shapes=[
            pltpu.VMEM((cache.shape[0], wide * wide + 8, channels), jnp.float32),
            pltpu.VMEM((cache.shape[0], rows, TAPS * TAPS * channels), jnp.bfloat16),
        ],
        compiler_params=pltpu.CompilerParams(vmem_limit_bytes=VMEM_LIMIT),
        name="context",
    )(place, cache, kernel, bias)


def section_kernel(
    shape, tick, place_ref, x_ref, sums_ref, part_ref, kernel_ref, bias_ref, gain_ref, offset_ref,
    kept_ref, next_ref, result_ref, out_sums_ref, act, held, cols, made,
):
    count, side, wide, _, pixels, members = shape
    rows_in = wide - 2 * tick
    rows_out = rows_in - 2
    channels = x_ref.shape[-1]
    flat_in = rows_in * wide
    flat_out = rows_out * wide
    halo = (wide - side) // 2
    flags = [place_ref[i] for i in range(4)]
    position = place_ref[4]

    @pl.when(position == tick)
    def _():
        mean_row = sums_ref[0:1] / pixels
        square_row = sums_ref[1:2] / pixels
        valid = masked(flags, halo - tick, rows_in, wide, side, channels)
        gain = gain_ref[...].reshape(1, channels)
        offset = offset_ref[...].reshape(1, channels)
        w0, w1, w2 = (kernel_ref[i] for i in range(TAPS))
        both_1 = jnp.concatenate([w1, w0], axis=1)
        both_2 = jnp.concatenate([w2, w1], axis=1)
        bias = bias_ref[...].reshape(1, channels)
        base = tick * (wide + 1)
        edge = halo - tick - 1
        sums, squares = [], []

        def prepare(f):
            mean = unpacked(mean_row, f, members)
            variance = jnp.maximum(unpacked(square_row, f, members) - mean * mean, 0.0)
            scale = gain / jnp.sqrt(variance + EPSILON)
            values = x_ref[f].astype(jnp.float32)
            held[f, :flat_in] = values
            normed = (values - mean) * scale + offset
            half = 0.5 * normed
            active = (half + half * jnp.tanh(half)).reshape(rows_in, wide, channels)
            active = jnp.where(valid, active, 0.0).reshape(flat_in, channels)
            act[f, :flat_in] = active
            unfold(act, cols, f, wide, flat_out, channels)

        def finish(g, value):
            new = value + held[g, wide + 1 : wide + 1 + flat_out]
            new = new.astype(jnp.bfloat16)
            made[g, :flat_out] = new.astype(jnp.float32)
            if next_ref is not None:
                next_ref[g] = new
            total_f = jnp.zeros((side, channels), jnp.float32)
            square_f = jnp.zeros((side, channels), jnp.float32)
            for y in range(side):
                at = (y + edge) * wide + edge
                row = made[g, at : at + side]
                if out_sums_ref is not None:
                    total_f = total_f + row
                    square_f = square_f + row * row
                result_ref[g, y] = row.astype(jnp.bfloat16)
            sums.append(jnp.sum(total_f, axis=0, keepdims=True))
            squares.append(jnp.sum(square_f, axis=0, keepdims=True))

        for f in range(0, count, 2):
            prepare(f)
            pair = matmul(cols, f, flat_out, both_2)
            first, second = pair[:, :channels], pair[:, channels:]
            if f == 0:
                finish(f, first + part_ref[0, base : base + flat_out])
                made[f + 1, :flat_out] = second + part_ref[1, base : base + flat_out]
            else:
                finish(f, first + made[f, :flat_out])
                made[f + 1, :flat_out] = made[f + 1, :flat_out] + second
            if f + 2 < count:
                made[f + 2, :flat_out] = matmul(cols, f, flat_out, w0) + bias
            prepare(f + 1)
            finish(f + 1, matmul(cols, f + 1, flat_out, w2) + made[f + 1, :flat_out])
            if f + 2 < count:
                pair = matmul(cols, f + 1, flat_out, both_1)
                made[f + 2, :flat_out] = made[f + 2, :flat_out] + pair[:, :channels]
                made[f + 3, :flat_out] = pair[:, channels:] + bias
        if out_sums_ref is not None:
            out_sums_ref[0:1, :] = packed(jnp.concatenate(sums, axis=0), members)
            out_sums_ref[1:2, :] = packed(jnp.concatenate(squares, axis=0), members)

    @pl.when(position != tick)
    def _():
        result_ref[...] = jnp.zeros_like(result_ref) if kept_ref is None else kept_ref[...]
        if out_sums_ref is not None:
            out_sums_ref[...] = jnp.zeros_like(out_sums_ref)


def section_step(shape, tick, place, x, sums, part, kernel, bias, gain, offset, kept):
    count, side, wide, sections, _, _ = shape
    channels = x.shape[-1]
    rows_out = wide - 2 * tick - 2
    last = tick == sections - 1
    vmem = pl.BlockSpec(memory_space=pltpu.VMEM)
    inputs = [place, x, sums, part, kernel, bias, gain, offset]
    if kept is not None:
        inputs.append(kept)
    outs = [jax.ShapeDtypeStruct((count, side, side, channels), jnp.bfloat16)]
    if not last:
        outs.insert(0, jax.ShapeDtypeStruct((count, rows_out * wide, channels), jnp.bfloat16))
        outs.append(jax.ShapeDtypeStruct((2, channels), jnp.float32))

    def body(*refs):
        refs = list(refs)
        given = refs[:8]
        del refs[:8]
        kept_ref = refs.pop(0) if kept is not None else None
        next_ref = refs.pop(0) if not last else None
        result_ref = refs.pop(0)
        out_sums_ref = refs.pop(0) if not last else None
        section_kernel(shape, tick, *given, kept_ref, next_ref, result_ref, out_sums_ref, *refs)

    full = wide * wide + 8
    return pl.pallas_call(
        body,
        out_shape=tuple(outs),
        in_specs=[pl.BlockSpec(memory_space=pltpu.SMEM)] + [vmem] * (len(inputs) - 1),
        out_specs=tuple([vmem] * len(outs)),
        scratch_shapes=[
            pltpu.VMEM((count, full, channels), jnp.float32),
            pltpu.VMEM((count, full, channels), jnp.float32),
            pltpu.VMEM((count, rows_out * wide, TAPS * TAPS * channels), jnp.bfloat16),
            pltpu.VMEM((count, rows_out * wide, channels), jnp.float32),
        ],
        compiler_params=pltpu.CompilerParams(vmem_limit_bytes=VMEM_LIMIT),
    )(*inputs)


def local(frames, cache, conv_weight, conv_bias, norm_gain, norm_bias):
    sections = lax.axis_size("section")
    tiles = lax.axis_size("tile")
    across = min(8, tiles // 2)
    down = tiles // across
    position = lax.axis_index("section")
    placed = (lax.axis_index("tile") + across + 2) % tiles
    column, row_at = placed % across, placed // across
    x = frames[:, 0]
    count, side, _, channels = x.shape
    members = channels // GROUPS
    halo = sections
    wide = side + 2 * halo
    pixels = float(side * side * members * tiles)
    shape = (count, side, wide, sections, pixels, members)
    flags = [row_at == 0, row_at == down - 1, column == 0, column == across - 1]
    place = jnp.stack([f.astype(jnp.int32) for f in flags] + [position.astype(jnp.int32)])
    kernel = conv_weight[0].reshape(TAPS, TAPS * TAPS * channels, channels)

    old = cache[0, :, 0]
    context = old.shape[0]
    seq = lax.optimization_barrier(jnp.concatenate([old, x], axis=0))
    left = shifted(seq[:, :, side - halo :], 1)
    right = shifted(seq[:, :, :halo], -1)
    sums = both_cores(first_sums(seq, count, members))
    left, right, sums = lax.optimization_barrier((left, right, sums))
    middle = jnp.concatenate([left, seq, right], axis=2)
    above = shifted(middle[:, side - halo :], across)
    below = shifted(middle[:, :halo], -across)
    sums = of_everyone(sums)
    held_cache, x = (
        jnp.concatenate([above[c], middle[c], below[c]], axis=1).reshape(-1, wide * wide, channels)
        for c in (slice(0, context), slice(context, None))
    )
    part = context_part(side, wide, place, held_cache, kernel, conv_bias)

    result = None
    for tick in range(sections):
        made = section_step(
            shape, tick, place, x, sums, part, kernel, conv_bias, norm_gain, norm_bias, result
        )
        if tick + 1 == sections:
            (result,) = made
            break
        x, result, sums = made
        hop = [(tick, tick + 1)]
        sums = to_next(sums, tick)
        x = lax.ppermute(x, "section", hop)
        sums = of_everyone(sums)
    return result[None, :, None]


def solution(mesh):
    placed = (
        P("parts", "tile", None, None, None),
        P("section", "parts", "tile", None, None, None),
        P("section", None, None, None, None, None),
        P("section", None),
        P("section", None),
        P("section", None),
    )
    return jax.shard_map(
        local,
        mesh=mesh,
        in_specs=placed,
        out_specs=P("section", "parts", "tile", None, None, None),
        check_vma=False,
    )
```
